512 devices in a mesh: dm: 16 (over z, core), tm: 32 (over x, y).
Axes of the slice: x: 4, y: 8, z: 8, core: 2. Of those that a mesh axis runs over, the one named last changes fastest.
Arguments:
- dispersed: float32 [4096, 32768], P('dm', 'tm')
- widths: int32 [4], replicated, may hold values from 1 to 129, as said below
Outputs:
- snr: bfloat16 [4, 4096, 32768], P(None, 'dm', 'tm')
- peaks: float32 [4, 4096], P(None, 'dm')
The draws below stay inside these ranges and needn't reach their ends.
Inputs may be any that keep to these rules, and one draw needn't show every extreme that they name: `widths`: at least one width equals 129.
All inputs are finite; a program needn't handle non-finite values.
Results may differ from the reference program's by a relative error of at most 0.001.
Values sent between devices are 32-bit elements; how exact they have to be, the bound alone decides.
A program may use at most 64 MiB of HBM per device.

```python
import math
import jax
import jax.numpy as jnp
from jax import lax

DM_DEV = 256
HALF = 128
WMAX = 129
NBOX = 4
TRIAL_MEASURES = 4096
TIME_SAMPLES = 32768


def draw_dispersed(key, part):
    random_key_list = jax.random.split(key, 8)
    trial_row_axis = jnp.arange(TRIAL_MEASURES, dtype=jnp.float32)[:, None]
    time_axis = jnp.arange(TIME_SAMPLES, dtype=jnp.float32)[None, :]
    row_spread_scale = jnp.exp(jax.random.uniform(random_key_list[0], (TRIAL_MEASURES, 1), jnp.float32) * math.log(10.0))
    sample_time_scale = jnp.exp(math.log(3.0) * time_axis / TIME_SAMPLES)
    random_perturbation = jax.random.normal(random_key_list[1], (TRIAL_MEASURES, TIME_SAMPLES), jnp.float32)
    offset_scale = 3.0
    pulse_level = 8.0
    offsets = jax.random.normal(random_key_list[2], (TRIAL_MEASURES, 1), jnp.float32) * offset_scale
    amplitude = jax.random.uniform(random_key_list[3], (TRIAL_MEASURES, 1), jnp.float32) * 5.0
    cycles = 1.0 + 3.0 * jax.random.uniform(random_key_list[4], (TRIAL_MEASURES, 1), jnp.float32)
    phase_shift = jax.random.uniform(random_key_list[5], (TRIAL_MEASURES, 1), jnp.float32) * 2.0 * math.pi
    slope_component = offsets + amplitude * jnp.sin(2.0 * math.pi * cycles * time_axis / TIME_SAMPLES + phase_shift)
    pulse_events = jnp.where(jax.random.uniform(random_key_list[6], (TIME_SAMPLES,), jnp.float32) < 0.02, jax.random.normal(random_key_list[7], (TIME_SAMPLES,), jnp.float32) * pulse_level, 0.0)
    pulse_gain = 1.0 + 2.0 * trial_row_axis / TRIAL_MEASURES
    return row_spread_scale * sample_time_scale * random_perturbation + slope_component + pulse_gain * pulse_events[None, :]


def draw_widths(key, part):
    random_key_list = jax.random.split(key, 2)
    width_draw = jax.random.randint(random_key_list[0], (NBOX,), 1, WMAX + 1, jnp.int32)
    chosen = jax.random.randint(random_key_list[1], (), 0, NBOX, jnp.int32)
    return jnp.where(jnp.arange(NBOX, dtype=jnp.int32) == chosen, WMAX, width_draw).astype(jnp.int32)


def setup_inputs(seed: int = 0) -> dict:
    arg_keys = jax.random.split(jax.random.key(seed), 3)
    return {
        "dispersed": draw_dispersed(jax.random.fold_in(arg_keys[2], 71), 0),
        "widths": draw_widths(jax.random.fold_in(arg_keys[2], 71), 0),
    }


eps_value = 1e-06

def band_table(span_list, block_len):
    column_idx = jnp.arange(span_list.shape[0] * block_len, dtype=jnp.int32)
    offsets = column_idx % block_len
    reaches = jnp.repeat(span_list, block_len)
    row_idx = jnp.arange(2 * block_len, dtype=jnp.int32)[:, None]
    inside = (row_idx >= offsets[None, :]) & (row_idx < offsets[None, :] + reaches[None, :])
    return inside.astype(jnp.float32)

def window_sum(extended, length, band_matrix, block_len):
    row_count = extended.shape[0]
    block_count = length // block_len
    blocks = extended[:, :length + block_len].reshape(row_count, block_count + 1, block_len)
    paired = jnp.concatenate([blocks[:, :-1], blocks[:, 1:]], axis=2)
    return jnp.einsum('rbs,sk->rbk', paired, band_matrix, precision=lax.Precision.HIGHEST)

def boxcar(extended, length, band_matrix, inverse, block_len):
    row_count = extended.shape[0]
    moving = window_sum(extended, length, band_matrix, block_len)
    moving = moving.reshape(row_count, length // block_len, inverse.shape[0], block_len)
    moving = jnp.transpose(moving, (2, 0, 1, 3)).reshape(inverse.shape[0], row_count, length)
    return moving * inverse[:, None, None]

def reference(dispersed, widths):
    row_total, total_len = dispersed.shape
    block_len = 2 * HALF
    ma_band = band_table(jnp.full((1,), 2 * HALF + 1, jnp.int32), block_len)
    box_band = band_table(widths, block_len)
    inverse = 1.0 / jnp.sqrt(widths.astype(jnp.float32))
    positions = jnp.arange(total_len, dtype=jnp.int32)
    counts = (jnp.minimum(positions + HALF, total_len - 1) - jnp.maximum(positions - HALF, 0) + 1).astype(jnp.float32)

    def detrend(row_block):
        row_count = row_block.shape[0]
        first_mean = window_sum(jnp.pad(row_block, ((0, 0), (HALF, HALF))), total_len, ma_band, block_len).reshape(row_count, total_len) / counts
        smooth_mean = window_sum(jnp.pad(first_mean, ((0, 0), (HALF, HALF))), total_len, ma_band, block_len).reshape(row_count, total_len) / counts
        return row_block - smooth_mean
    grouped = dispersed.reshape(row_total // DM_DEV, DM_DEV, total_len)
    detrended = lax.map(detrend, grouped).reshape(row_total, total_len)
    power_sum = lax.optimization_barrier(jnp.sum(detrended * detrended, axis=1))
    row_spread_scale = jnp.sqrt(power_sum / total_len + eps_value)
    normed = detrended / row_spread_scale[:, None]
    common = lax.optimization_barrier(jnp.sum(normed, axis=0)) / row_total
    cleaned = normed - common[None, :]

    def filtered(row_block):
        series = boxcar(jnp.pad(row_block, ((0, 0), (0, block_len))), total_len, box_band, inverse, block_len)
        return (series.astype(jnp.bfloat16), lax.optimization_barrier(jnp.max(series, axis=2)))
    series, peak_values = lax.map(filtered, cleaned.reshape(row_total // DM_DEV, DM_DEV, total_len))
    snr = jnp.transpose(series, (1, 0, 2, 3)).reshape(NBOX, row_total, total_len)
    peaks = jnp.transpose(peak_values, (1, 0, 2)).reshape(NBOX, row_total)
    return (snr, peaks)
```

```python
import functools

import jax
import jax.numpy as jnp
from jax import lax
from jax.experimental import pallas as pl
from jax.experimental.pallas import tpu as pltpu
from jax.sharding import PartitionSpec as P

MESH = pl.DeviceIdType.MESH
HALF = 128
BLOCK = 2 * HALF
EPS = 1e-06
CHUNKS = 4


def parts_of(x):
    high = x.astype(jnp.bfloat16)
    rest = x - high.astype(jnp.float32)
    mid = rest.astype(jnp.bfloat16)
    low = (rest - mid.astype(jnp.float32)).astype(jnp.bfloat16)
    return high, mid, low


def banded(x, band):
    return jnp.dot(jnp.concatenate(parts_of(x), axis=1), band, preferred_element_type=jnp.float32)


def peer_offsets(peers):
    side = 8 if peers % 8 == 0 else peers
    other = peers // side
    steps = [(dx, dy) for dx in range(other) for dy in range(side) if dx or dy]
    reach = lambda s: min(s[0], other - s[0]) + min(s[1], side - s[1])
    return side, other, sorted(steps, key=reach, reverse=True)


def kernel(
    tm_size, dm_size, widths, x, snr, peaks,
    ext, low_band, high_band, box_band, fm, part, det, split, boxed, out, rows_max,
    power_out, power_in, scale, col_out, col_in, common, box_common, peak_out, peak_in,
    load_sem, halo_send, halo_recv, head_send, head_recv,
    power_send, power_recv, col_send, col_recv, peak_send, peak_recv, store_sem,
):
    rows, length = x.shape
    boxes = widths.shape[0]
    blocks = length // BLOCK
    tiles = length // HALF
    total_len = length * tm_size
    tm = lax.axis_index("tm")
    dm = lax.axis_index("dm")
    right, left = lax.rem(tm + 1, tm_size), lax.rem(tm + tm_size - 1, tm_size)
    side, other, steps = peer_offsets(tm_size)
    tm_x, tm_y = tm // side, tm % side

    def tm_peer(step):
        return lax.rem(tm_x + step[0], other) * side + lax.rem(tm_y + step[1], side)

    dm_steps = sorted(range(1, dm_size), key=lambda d: min(d, dm_size - d), reverse=True)

    barrier = pltpu.get_barrier_semaphore()
    for step in steps:
        pl.semaphore_signal(barrier, inc=1, device_id={"tm": tm_peer(step)}, device_id_type=MESH)
    for d in dm_steps:
        pl.semaphore_signal(
            barrier, inc=1, device_id={"dm": lax.rem(dm + d, dm_size)}, device_id_type=MESH
        )
    loads = {}
    for b in [1, blocks] + list(range(2, blocks)):
        loads[b] = pltpu.make_async_copy(
            x.at[:, pl.ds((b - 1) * BLOCK, BLOCK)], ext.at[b], load_sem.at[b - 1]
        )
        loads[b].start()

    row_idx = lax.broadcasted_iota(jnp.int32, (BLOCK, BLOCK), 0)
    col_idx = lax.broadcasted_iota(jnp.int32, (BLOCK, BLOCK), 1)
    low = (row_idx >= col_idx).astype(jnp.float32).astype(jnp.bfloat16)
    high = (row_idx <= col_idx).astype(jnp.float32).astype(jnp.bfloat16)
    lane = lax.broadcasted_iota(jnp.int32, (BLOCK, HALF), 1)
    depth = lax.broadcasted_iota(jnp.int32, (BLOCK, HALF), 0)
    for k in range(3):
        low_band[pl.ds(k * BLOCK, BLOCK), :] = low
        high_band[pl.ds(k * BLOCK, BLOCK), :] = high
    for i in range(boxes):
        inside = (depth >= lane) & (depth < lane + widths[i])
        for k in range(3):
            box_band[pl.ds(k * BLOCK, BLOCK), pl.ds(i * HALF, HALF)] = inside.astype(
                jnp.float32
            ).astype(jnp.bfloat16)

    def inverse_counts(first):
        pos = first + lax.broadcasted_iota(jnp.int32, (1, BLOCK), 1)
        counts = (jnp.minimum(pos + HALF, total_len - 1) - jnp.maximum(pos - HALF, 0) + 1)
        valid = (pos >= 0) & (pos < total_len)
        return jnp.where(valid, 1.0 / jnp.maximum(counts, 1).astype(jnp.float32), 0.0)

    offset = tm * length
    inner = 1.0 / (2 * HALF + 1)
    edge_first = inverse_counts(offset - HALF)
    edge_last = inverse_counts(offset + length - HALF)
    own_first = inverse_counts(offset)
    own_last = inverse_counts(offset + length - BLOCK)

    loads[1].wait()
    loads[blocks].wait()
    pl.semaphore_wait(barrier, len(steps) + len(dm_steps))
    chunk = rows // CHUNKS
    halos = []
    for q in range(CHUNKS):
        span = pl.ds(q * chunk, chunk)
        to_right = pltpu.make_async_remote_copy(
            src_ref=ext.at[blocks, span], dst_ref=ext.at[0, span],
            send_sem=halo_send.at[0, q], recv_sem=halo_recv.at[0, q],
            device_id={"tm": right}, device_id_type=MESH,
        )
        to_left = pltpu.make_async_remote_copy(
            src_ref=ext.at[1, span], dst_ref=ext.at[blocks + 1, span],
            send_sem=halo_send.at[1, q], recv_sem=halo_recv.at[1, q],
            device_id={"tm": left}, device_id_type=MESH,
        )
        to_right.start()
        to_left.start()
        halos.append((to_right, to_left))

    for b in range(2, blocks):
        loads[b].wait()
    part[0] = banded(ext[1], high_band[...])
    part[1] = banded(ext[blocks], low_band[...])
    for b in range(1, blocks):
        sums = banded(ext[b], low_band[...]) + banded(ext[b + 1], high_band[...])
        fm[b] = sums * inner
    part[2] = banded(fm[1], high_band[...])
    part[3] = banded(fm[blocks - 1], low_band[...])

    def keep(block_idx, span, values):
        for k, piece in enumerate(parts_of(values)):
            split[k, span, pl.ds(block_idx * BLOCK, BLOCK)] = piece
        det[span, pl.ds(block_idx * BLOCK, BLOCK)] = values
        squares = values * values
        return squares[:, :HALF] + squares[:, HALF:]

    power = jnp.zeros((rows, HALF), jnp.float32)
    for b in range(1, blocks - 1):
        smooth = (banded(fm[b], low_band[...]) + banded(fm[b + 1], high_band[...])) * inner
        power = power + keep(b, pl.ds(0, rows), ext[b + 1] - smooth)
    rows_max[0] = power

    def box_sums(t):
        window = jnp.concatenate(
            [split[k, :, pl.ds(t * HALF, BLOCK)] for k in range(3)], axis=1
        )
        boxed[t] = jnp.dot(window, box_band[...], preferred_element_type=jnp.float32)

    early = range(BLOCK // HALF, tiles - 3)
    for t in early:
        box_sums(t)

    is_first = tm == 0
    is_last = tm == tm_size - 1
    for q in range(CHUNKS):
        span = pl.ds(q * chunk, chunk)
        halos[q][0].wait_recv()
        before = jnp.where(is_first, 0.0, ext[0, span])
        mean = (part[0, span] + banded(before, low_band[...])) * edge_first
        smooth = (part[2, span] + banded(mean, low_band[...])) * own_first
        power = keep(0, span, ext[1, span] - smooth)
        halos[q][1].wait_recv()
        after = jnp.where(is_last, 0.0, ext[blocks + 1, span])
        mean = (part[1, span] + banded(after, high_band[...])) * edge_last
        smooth = (part[3, span] + banded(mean, high_band[...])) * own_last
        power = power + keep(blocks - 1, span, ext[blocks, span] - smooth)
        rows_max[0, span] = rows_max[0, span] + power

    for h in range(rows // HALF):
        turned = rows_max[0, pl.ds(h * HALF, HALF)].T
        power_out[pl.ds(h, 1), :] = jnp.sum(turned, axis=0, keepdims=True)

    def to_peers(src, dst, send_sem, recv_sem):
        for step in steps:
            pltpu.make_async_remote_copy(
                src_ref=src, dst_ref=dst.at[step[0] * side + step[1] - 1],
                send_sem=send_sem, recv_sem=recv_sem,
                device_id={"tm": tm_peer(step)}, device_id_type=MESH,
            ).start()

    to_peers(power_out, power_in, power_send, power_recv)
    head = pltpu.make_async_remote_copy(
        src_ref=det.at[:, pl.ds(0, HALF)], dst_ref=det.at[:, pl.ds(length, HALF)],
        send_sem=head_send, recv_sem=head_recv,
        device_id={"tm": left}, device_id_type=MESH,
    )
    head.start()

    for t in range(tiles - 1):
        if t not in early:
            box_sums(t)
    pltpu.make_async_copy(power_in, power_in, power_recv).wait()
    totals = power_out[...] + jnp.sum(power_in[...], axis=0)
    inverse_scale = 1.0 / jnp.sqrt(totals * (1.0 / total_len) + EPS)
    for h in range(rows // HALF):
        row = jnp.broadcast_to(inverse_scale[h:h + 1, :], (HALF, HALF))
        scale[pl.ds(h * HALF, HALF), :] = row.T

    head.wait_recv()
    head_values = jnp.where(is_last, 0.0, det[:, pl.ds(length, HALF)])

    def column_sum(values):
        weighted = (values * scale[...]).reshape(rows // 8, 8, HALF)
        return jnp.sum(jnp.sum(weighted, axis=0), axis=0, keepdims=True)

    for t in range(tiles):
        col_out[pl.ds(t, 1), :] = column_sum(det[:, pl.ds(t * HALF, HALF)])
    col_out[pl.ds(tiles, 1), :] = column_sum(head_values)
    for d in dm_steps:
        pltpu.make_async_remote_copy(
            src_ref=col_out, dst_ref=col_in.at[d - 1], send_sem=col_send, recv_sem=col_recv,
            device_id={"dm": lax.rem(dm + d, dm_size)}, device_id_type=MESH,
        ).start()

    for k, piece in enumerate(parts_of(head_values)):
        split[k, :, pl.ds(length, HALF)] = piece
    box_sums(tiles - 1)

    inverse = []
    for i in range(boxes):
        width = jnp.full((16, HALF), widths[i], jnp.int32).astype(jnp.float32)
        inverse.append(1.0 / jnp.sqrt(width))

    pltpu.make_async_copy(col_in, col_in, col_recv).wait()
    column_total = col_out[...] + jnp.sum(col_in[...], axis=0)
    common[...] = column_total * (1.0 / (rows * dm_size))
    window = jnp.concatenate([common[pl.ds(0, tiles), :], common[pl.ds(1, tiles), :]], axis=1)
    box_common[...] = banded(window, box_band[...])

    stores = []
    for i in range(boxes):
        offsets = [
            jnp.broadcast_to(box_common[pl.ds(t, 1), pl.ds(i * HALF, HALF)], (16, HALF)) * inverse[i]
            for t in range(tiles)
        ]

        def some_rows(r, carry):
            span = pl.ds(pl.multiple_of(r * 16, 16), 16)
            gain = scale[span, :] * inverse[i]
            most = None
            for t in range(tiles):
                series = boxed[t, span, pl.ds(i * HALF, HALF)] * gain - offsets[t]
                most = series if most is None else jnp.maximum(most, series)
                out[i, span, pl.ds(t * HALF, HALF)] = series.astype(jnp.bfloat16)
            rows_max[i, span] = most
            return carry

        lax.fori_loop(0, rows // 16, some_rows, 0)
        stores.append(pltpu.make_async_copy(out.at[i], snr.at[i], store_sem.at[i]))
        stores[-1].start()

    halves = rows // HALF
    for i in range(boxes):
        for h in range(halves):
            turned = rows_max[i, pl.ds(h * HALF, HALF)].T
            peak_out[pl.ds(i * halves + h, 1), :] = jnp.max(turned, axis=0, keepdims=True)
    to_peers(peak_out, peak_in, peak_send, peak_recv)
    pltpu.make_async_copy(peak_in, peak_in, peak_recv).wait()
    most = jnp.maximum(peak_out[...], jnp.max(peak_in[...], axis=0))
    for i in range(boxes):
        for h in range(halves):
            row = i * halves + h
            peaks[pl.ds(i, 1), pl.ds(h * HALF, HALF)] = most[row:row + 1, :]

    for to_right, to_left in halos:
        to_right.wait_send()
        to_left.wait_send()
    head.wait_send()
    pltpu.make_async_copy(power_in, power_in, power_send).wait()
    pltpu.make_async_copy(col_in, col_in, col_send).wait()
    pltpu.make_async_copy(peak_in, peak_in, peak_send).wait()
    for store in stores:
        store.wait()


def solution(mesh):
    tm_size, dm_size = mesh.shape["tm"], mesh.shape["dm"]

    def step(dispersed, widths):
        rows, length = dispersed.shape
        boxes = widths.shape[0]
        blocks, tiles, halves = length // BLOCK, length // HALF, rows // HALF
        f32, bf16 = jnp.float32, jnp.bfloat16
        dma = pltpu.SemaphoreType.DMA
        return pl.pallas_call(
            functools.partial(kernel, tm_size, dm_size),
            out_shape=(
                jax.ShapeDtypeStruct((boxes, rows, length), bf16),
                jax.ShapeDtypeStruct((boxes, rows), f32),
            ),
            in_specs=[
                pl.BlockSpec(memory_space=pltpu.SMEM),
                pl.BlockSpec(memory_space=pl.ANY),
            ],
            out_specs=(
                pl.BlockSpec(memory_space=pl.ANY),
                pl.BlockSpec(memory_space=pltpu.VMEM),
            ),
            scratch_shapes=[
                pltpu.VMEM((blocks + 2, rows, BLOCK), f32),
                pltpu.VMEM((3 * BLOCK, BLOCK), bf16),
                pltpu.VMEM((3 * BLOCK, BLOCK), bf16),
                pltpu.VMEM((3 * BLOCK, boxes * HALF), bf16),
                pltpu.VMEM((blocks, rows, BLOCK), f32),
                pltpu.VMEM((4, rows, BLOCK), f32),
                pltpu.VMEM((rows, length + HALF), f32),
                pltpu.VMEM((3, rows, length + HALF), bf16),
                pltpu.VMEM((tiles, rows, boxes * HALF), f32),
                pltpu.VMEM((boxes, rows, length), bf16),
                pltpu.VMEM((boxes, rows, HALF), f32),
                pltpu.VMEM((halves, HALF), f32),
                pltpu.VMEM((tm_size - 1, halves, HALF), f32),
                pltpu.VMEM((rows, HALF), f32),
                pltpu.VMEM((tiles + 1, HALF), f32),
                pltpu.VMEM((dm_size - 1, tiles + 1, HALF), f32),
                pltpu.VMEM((tiles + 1, HALF), f32),
                pltpu.VMEM((tiles, boxes * HALF), f32),
                pltpu.VMEM((boxes * halves, HALF), f32),
                pltpu.VMEM((tm_size - 1, boxes * halves, HALF), f32),
                dma((blocks,)),
                dma((2, CHUNKS)),
                dma((2, CHUNKS)),
                dma, dma, dma, dma, dma, dma, dma, dma,
                dma((boxes,)),
            ],
            compiler_params=pltpu.CompilerParams(
                collective_id=0, has_side_effects=True, vmem_limit_bytes=48 * 2**20
            ),
        )(widths, dispersed)

    return jax.shard_map(
        step,
        mesh=mesh,
        in_specs=(P("dm", "tm"), P()),
        out_specs=(P(None, "dm", "tm"), P(None, "dm")),
        check_vma=False,
    )
```

```python
import functools

import jax
import jax.numpy as jnp
from jax import lax
from jax.experimental import pallas as pl
from jax.experimental.pallas import tpu as pltpu
from jax.sharding import PartitionSpec as P

MESH = pl.DeviceIdType.MESH
HALF = 128
BLOCK = 2 * HALF
EPS = 1e-06
CHUNKS = 4


def parts_of(x):
    high = x.astype(jnp.bfloat16)
    rest = x - high.astype(jnp.float32)
    mid = rest.astype(jnp.bfloat16)
    low = (rest - mid.astype(jnp.float32)).astype(jnp.bfloat16)
    return high, mid, low


def banded(x, band):
    rows = x.shape[0]
    stacked = jnp.concatenate(parts_of(x), axis=0)
    sums = jnp.dot(stacked, band, preferred_element_type=jnp.float32)
    return sums[:rows] + sums[rows:2 * rows] + sums[2 * rows:]


def peer_offsets(peers):
    side = 8 if peers % 8 == 0 else peers
    other = peers // side
    steps = [(dx, dy) for dx in range(other) for dy in range(side) if dx or dy]
    reach = lambda s: min(s[0], other - s[0]) + min(s[1], side - s[1])
    return side, other, sorted(steps, key=reach, reverse=True)


def kernel(
    tm_size, dm_size, widths_in, x, snr, peaks,
    widths, widths_sem, ext, low_band, high_band, box_band, fm, part, det, split, boxed, rows_max,
    power_out, power_in, scale, col_out, col_in, common, box_common, peak_out, peak_in,
    load_sem, halo_send, halo_recv, head_send, head_recv,
    power_send, power_recv, col_send, col_recv, peak_send, peak_recv, dm_known, tm_tokens, dm_tokens,
):
    rows, length = x.shape
    boxes = widths.shape[0]
    blocks = length // BLOCK
    tiles = length // HALF
    total_len = length * tm_size
    tm = lax.axis_index("tm")
    dm = lax.axis_index("dm")
    right, left = lax.rem(tm + 1, tm_size), lax.rem(tm + tm_size - 1, tm_size)
    side, other, steps = peer_offsets(tm_size)
    tm_x, tm_y = tm // side, tm % side

    def tm_peer(step):
        return lax.rem(tm_x + step[0], other) * side + lax.rem(tm_y + step[1], side)

    dm_steps = sorted(range(1, dm_size), key=lambda d: min(d, dm_size - d), reverse=True)

    barrier = pltpu.get_barrier_semaphore()
    near = sorted({1, tm_size - 1})
    for d in near:
        pl.semaphore_signal(
            barrier, inc=1, device_id={"tm": lax.rem(tm + d, tm_size)}, device_id_type=MESH
        )

    @pl.when(dm < dm_size - 1)
    def _():
        pl.semaphore_signal(barrier, inc=1, device_id={"dm": dm + 1}, device_id_type=MESH)

    fetch = pltpu.make_async_copy(widths_in, widths, widths_sem)
    fetch.start()
    loads = {}
    for b in [1, blocks] + list(range(2, blocks)):
        loads[b] = pltpu.make_async_copy(
            x.at[:, pl.ds((b - 1) * BLOCK, BLOCK)], ext.at[b], load_sem.at[b - 1]
        )
        loads[b].start()

    tm_rounds = [d for d in (1, 2, 4, 8, 16, 32) if 2 * d < tm_size]
    dm_rounds = [d for d in (1, 2, 4, 8, 16, 32) if d < dm_size - 1]

    def tm_tell(n):
        if n < len(tm_rounds):
            for d in {tm_rounds[n], tm_size - tm_rounds[n]}:
                pl.semaphore_signal(
                    tm_tokens.at[n], inc=1, device_id={"tm": lax.rem(tm + d, tm_size)},
                    device_id_type=MESH,
                )

    def tm_hear(n):
        if n < len(tm_rounds):
            pl.semaphore_wait(tm_tokens.at[n], len({tm_rounds[n], tm_size - tm_rounds[n]}))

    def dm_tell(n):
        if n < len(dm_rounds):
            d = dm_rounds[n]

            @pl.when(dm + d < dm_size)
            def _():
                pl.semaphore_signal(
                    dm_tokens.at[n], inc=1, device_id={"dm": dm + d}, device_id_type=MESH
                )

            @pl.when(dm >= d)
            def _():
                pl.semaphore_signal(
                    dm_tokens.at[n], inc=1, device_id={"dm": dm - d}, device_id_type=MESH
                )

    def dm_hear(n):
        if n < len(dm_rounds):
            d = dm_rounds[n]
            ahead = jnp.minimum((dm_size - 1 - dm) // d, 1)
            pl.semaphore_wait(dm_tokens.at[n], ahead + jnp.minimum(dm // d, 1))

    row_idx = lax.broadcasted_iota(jnp.int32, (BLOCK, BLOCK), 0)
    col_idx = lax.broadcasted_iota(jnp.int32, (BLOCK, BLOCK), 1)
    low = (row_idx >= col_idx).astype(jnp.float32).astype(jnp.bfloat16)
    high = (row_idx <= col_idx).astype(jnp.float32).astype(jnp.bfloat16)
    lane = lax.broadcasted_iota(jnp.int32, (BLOCK, HALF), 1)
    depth = lax.broadcasted_iota(jnp.int32, (BLOCK, HALF), 0)
    low_band[...] = low
    high_band[...] = high
    fetch.wait()
    for i in range(boxes):
        inside = (depth >= lane) & (depth < lane + widths[i])
        for k in range(3):
            box_band[pl.ds(k * BLOCK, BLOCK), pl.ds(i * HALF, HALF)] = inside.astype(
                jnp.float32
            ).astype(jnp.bfloat16)

    def inverse_counts(first):
        pos = first + lax.broadcasted_iota(jnp.int32, (1, BLOCK), 1)
        counts = (jnp.minimum(pos + HALF, total_len - 1) - jnp.maximum(pos - HALF, 0) + 1)
        valid = (pos >= 0) & (pos < total_len)
        return jnp.where(valid, 1.0 / jnp.maximum(counts, 1).astype(jnp.float32), 0.0)

    offset = tm * length
    inner = 1.0 / (2 * HALF + 1)
    edge_first = inverse_counts(offset - HALF)
    edge_last = inverse_counts(offset + length - HALF)
    own_first = inverse_counts(offset)
    own_last = inverse_counts(offset + length - BLOCK)

    loads[1].wait()
    loads[blocks].wait()
    pl.semaphore_wait(barrier, len(near) + jnp.minimum(dm, 1))
    chunk = rows // CHUNKS
    halos = []
    for q in range(CHUNKS):
        span = pl.ds(q * chunk, chunk)
        to_right = pltpu.make_async_remote_copy(
            src_ref=ext.at[blocks, span], dst_ref=ext.at[0, span],
            send_sem=halo_send.at[0, q], recv_sem=halo_recv.at[0, q],
            device_id={"tm": right}, device_id_type=MESH,
        )
        to_left = pltpu.make_async_remote_copy(
            src_ref=ext.at[1, span], dst_ref=ext.at[blocks + 1, span],
            send_sem=halo_send.at[1, q], recv_sem=halo_recv.at[1, q],
            device_id={"tm": left}, device_id_type=MESH,
        )
        to_right.start()
        to_left.start()
        halos.append((to_right, to_left))

    @pl.when(dm > 0)
    def _():
        pl.semaphore_signal(dm_known, inc=1, device_id={"dm": dm - 1}, device_id_type=MESH)

    tm_tell(0)

    for b in range(2, blocks):
        loads[b].wait()
    part[0] = banded(ext[1], high_band[...])
    part[1] = banded(ext[blocks], low_band[...])
    for b in range(1, blocks):
        sums = banded(ext[b], low_band[...]) + banded(ext[b + 1], high_band[...])
        fm[b] = sums * inner
        if b == 1:
            tm_hear(0)
            tm_tell(1)

    @pl.when(dm < dm_size - 1)
    def _():
        pl.semaphore_wait(dm_known, 1)

    dm_tell(0)
    part[2] = banded(fm[1], high_band[...])
    part[3] = banded(fm[blocks - 1], low_band[...])

    def keep(block_idx, span, values):
        for k, piece in enumerate(parts_of(values)):
            split[k, span, pl.ds(block_idx * BLOCK, BLOCK)] = piece
        det[span, pl.ds(block_idx * BLOCK, BLOCK)] = values
        squares = values * values
        return squares[:, :HALF] + squares[:, HALF:]

    power = jnp.zeros((rows, HALF), jnp.float32)
    for b in range(1, blocks - 1):
        smooth = (banded(fm[b], low_band[...]) + banded(fm[b + 1], high_band[...])) * inner
        power = power + keep(b, pl.ds(0, rows), ext[b + 1] - smooth)
    rows_max[0] = power
    tm_hear(1)
    tm_tell(2)

    def box_sums(t):
        window = jnp.concatenate(
            [split[k, :, pl.ds(t * HALF, BLOCK)] for k in range(3)], axis=1
        )
        boxed[t] = jnp.dot(window, box_band[...], preferred_element_type=jnp.float32)

    early = range(BLOCK // HALF, tiles - 3)
    for t in early:
        box_sums(t)

    is_first = tm == 0
    is_last = tm == tm_size - 1
    for q in range(CHUNKS):
        span = pl.ds(q * chunk, chunk)
        halos[q][0].wait_recv()
        halos[q][1].wait_recv()
        before = jnp.where(is_first, 0.0, ext[0, span])
        mean = (part[0, span] + banded(before, low_band[...])) * edge_first
        smooth = (part[2, span] + banded(mean, low_band[...])) * own_first
        after = jnp.where(is_last, 0.0, ext[blocks + 1, span])
        mean_after = (part[1, span] + banded(after, high_band[...])) * edge_last
        smooth_after = (part[3, span] + banded(mean_after, high_band[...])) * own_last
        power = keep(0, span, ext[1, span] - smooth)
        power = power + keep(blocks - 1, span, ext[blocks, span] - smooth_after)
        rows_max[0, span] = rows_max[0, span] + power
        if q == 1:
            tm_hear(2)
            tm_tell(3)

    for h in range(rows // HALF):
        turned = rows_max[0, pl.ds(h * HALF, HALF)].T
        power_out[pl.ds(h, 1), :] = jnp.sum(turned, axis=0, keepdims=True)

    for n in range(3, len(tm_rounds)):
        tm_hear(n)
        tm_tell(n + 1)

    def to_peers(src, dst, send_sem, recv_sem):
        for step in steps:
            pltpu.make_async_remote_copy(
                src_ref=src, dst_ref=dst.at[step[0] * side + step[1] - 1],
                send_sem=send_sem, recv_sem=recv_sem,
                device_id={"tm": tm_peer(step)}, device_id_type=MESH,
            ).start()

    to_peers(power_out, power_in, power_send, power_recv)
    head = pltpu.make_async_remote_copy(
        src_ref=det.at[:, pl.ds(0, HALF)], dst_ref=det.at[:, pl.ds(length, HALF)],
        send_sem=head_send, recv_sem=head_recv,
        device_id={"tm": left}, device_id_type=MESH,
    )
    head.start()

    for t in range(tiles - 1):
        if t not in early:
            box_sums(t)
    for n in range(len(dm_rounds)):
        dm_hear(n)
        dm_tell(n + 1)
    pltpu.make_async_copy(power_in, power_in, power_recv).wait()
    totals = power_out[...] + jnp.sum(power_in[...], axis=0)
    inverse_scale = 1.0 / jnp.sqrt(totals * (1.0 / total_len) + EPS)
    for h in range(rows // HALF):
        row = jnp.broadcast_to(inverse_scale[h:h + 1, :], (HALF, HALF))
        scale[pl.ds(h * HALF, HALF), :] = row.T

    head.wait_recv()
    head_values = jnp.where(is_last, 0.0, det[:, pl.ds(length, HALF)])

    def column_sum(values):
        weighted = (values * scale[...]).reshape(rows // 8, 8, HALF)
        return jnp.sum(jnp.sum(weighted, axis=0), axis=0, keepdims=True)

    for t in range(tiles):
        col_out[pl.ds(t, 1), :] = column_sum(det[:, pl.ds(t * HALF, HALF)])
    col_out[pl.ds(tiles, 1), :] = column_sum(head_values)
    for d in dm_steps:
        pltpu.make_async_remote_copy(
            src_ref=col_out, dst_ref=col_in.at[d - 1], send_sem=col_send, recv_sem=col_recv,
            device_id={"dm": lax.rem(dm + d, dm_size)}, device_id_type=MESH,
        ).start()

    for k, piece in enumerate(parts_of(head_values)):
        split[k, :, pl.ds(length, HALF)] = piece
    box_sums(tiles - 1)

    inverse = []
    for i in range(boxes):
        width = jnp.full((16, HALF), widths[i], jnp.int32).astype(jnp.float32)
        inverse.append(1.0 / jnp.sqrt(width))

    pltpu.make_async_copy(col_in, col_in, col_recv).wait()
    column_total = col_out[...] + jnp.sum(col_in[...], axis=0)
    common[...] = column_total * (1.0 / (rows * dm_size))
    window = jnp.concatenate([common[pl.ds(0, tiles), :], common[pl.ds(1, tiles), :]], axis=1)
    box_common[...] = banded(window, box_band[pl.ds(0, BLOCK), :])

    for i in range(boxes):
        offsets = [
            jnp.broadcast_to(box_common[pl.ds(t, 1), pl.ds(i * HALF, HALF)], (16, HALF)) * inverse[i]
            for t in range(tiles)
        ]

        def some_rows(r, carry):
            span = pl.ds(pl.multiple_of(r * 16, 16), 16)
            gain = scale[span, :] * inverse[i]
            most = None
            for t in range(tiles):
                series = boxed[t, span, pl.ds(i * HALF, HALF)] * gain - offsets[t]
                most = series if most is None else jnp.maximum(most, series)
                snr[i, span, pl.ds(t * HALF, HALF)] = series.astype(jnp.bfloat16)
            rows_max[i, span] = most
            return carry

        lax.fori_loop(0, rows // 16, some_rows, 0)

    halves = rows // HALF
    for i in range(boxes):
        for h in range(halves):
            turned = rows_max[i, pl.ds(h * HALF, HALF)].T
            peak_out[pl.ds(i * halves + h, 1), :] = jnp.max(turned, axis=0, keepdims=True)
    to_peers(peak_out, peak_in, peak_send, peak_recv)
    pltpu.make_async_copy(peak_in, peak_in, peak_recv).wait()
    most = jnp.maximum(peak_out[...], jnp.max(peak_in[...], axis=0))
    for i in range(boxes):
        for h in range(halves):
            row = i * halves + h
            peaks[pl.ds(i, 1), pl.ds(h * HALF, HALF)] = most[row:row + 1, :]

    for to_right, to_left in halos:
        to_right.wait_send()
        to_left.wait_send()
    head.wait_send()
    pltpu.make_async_copy(power_in, power_in, power_send).wait()
    pltpu.make_async_copy(col_in, col_in, col_send).wait()
    pltpu.make_async_copy(peak_in, peak_in, peak_send).wait()


def hand_out(snr, peaks, snr_out, peaks_out, sems):
    boxes = snr.shape[0]
    copies = [pltpu.make_async_copy(peaks, peaks_out, sems.at[boxes])]
    copies += [pltpu.make_async_copy(snr.at[i], snr_out.at[i], sems.at[i]) for i in range(boxes)]
    for copy in copies:
        copy.start()
    for copy in copies:
        copy.wait()


def solution(mesh):
    tm_size, dm_size = mesh.shape["tm"], mesh.shape["dm"]

    def step(dispersed, widths):
        rows, length = dispersed.shape
        boxes = widths.shape[0]
        blocks, tiles, halves = length // BLOCK, length // HALF, rows // HALF
        f32, bf16 = jnp.float32, jnp.bfloat16
        dma = pltpu.SemaphoreType.DMA
        inputs = [pltpu.with_memory_space_constraint(a, pltpu.HBM) for a in (widths, dispersed)]
        snr, peaks = pl.pallas_call(
            functools.partial(kernel, tm_size, dm_size),
            out_shape=(
                pltpu.VMEM((boxes, rows, length), bf16),
                pltpu.VMEM((boxes, rows), f32),
            ),
            in_specs=[pl.BlockSpec(memory_space=pltpu.HBM)] * 2,
            out_specs=(pl.BlockSpec(memory_space=pltpu.VMEM),) * 2,
            scratch_shapes=[
                pltpu.SMEM((boxes,), jnp.int32),
                dma,
                pltpu.VMEM((blocks + 2, rows, BLOCK), f32),
                pltpu.VMEM((BLOCK, BLOCK), bf16),
                pltpu.VMEM((BLOCK, BLOCK), bf16),
                pltpu.VMEM((3 * BLOCK, boxes * HALF), bf16),
                pltpu.VMEM((blocks, rows, BLOCK), f32),
                pltpu.VMEM((4, rows, BLOCK), f32),
                pltpu.VMEM((rows, length + HALF), f32),
                pltpu.VMEM((3, rows, length + HALF), bf16),
                pltpu.VMEM((tiles, rows, boxes * HALF), f32),
                pltpu.VMEM((boxes, rows, HALF), f32),
                pltpu.VMEM((halves, HALF), f32),
                pltpu.VMEM((tm_size - 1, halves, HALF), f32),
                pltpu.VMEM((rows, HALF), f32),
                pltpu.VMEM((tiles + 1, HALF), f32),
                pltpu.VMEM((dm_size - 1, tiles + 1, HALF), f32),
                pltpu.VMEM((tiles + 1, HALF), f32),
                pltpu.VMEM((tiles, boxes * HALF), f32),
                pltpu.VMEM((boxes * halves, HALF), f32),
                pltpu.VMEM((tm_size - 1, boxes * halves, HALF), f32),
                dma((blocks,)),
                dma((2, CHUNKS)),
                dma((2, CHUNKS)),
                dma, dma, dma, dma, dma, dma, dma, dma,
                pltpu.SemaphoreType.REGULAR,
                pltpu.SemaphoreType.REGULAR((5,)),
                pltpu.SemaphoreType.REGULAR((5,)),
            ],
            compiler_params=pltpu.CompilerParams(
                collective_id=0, has_side_effects=True, vmem_limit_bytes=48 * 2**20
            ),
        )(*inputs)
        return pl.pallas_call(
            hand_out,
            out_shape=(
                jax.ShapeDtypeStruct(snr.shape, bf16),
                jax.ShapeDtypeStruct(peaks.shape, f32),
            ),
            in_specs=[pl.BlockSpec(memory_space=pl.ANY)] * 2,
            out_specs=(pl.BlockSpec(memory_space=pl.ANY),) * 2,
            scratch_shapes=[dma((boxes + 1,))],
            compiler_params=pltpu.CompilerParams(vmem_limit_bytes=2**22),
        )(snr, peaks)

    return jax.shard_map(
        step,
        mesh=mesh,
        in_specs=(P("dm", "tm"), P()),
        out_specs=(P(None, "dm", "tm"), P(None, "dm")),
        check_vma=False,
    )
```

```python
import functools

import jax
import jax.numpy as jnp
from jax import lax
from jax.experimental import pallas as pl
from jax.experimental.pallas import tpu as pltpu
from jax.sharding import PartitionSpec as P

MESH = pl.DeviceIdType.MESH
HALF = 128
BLOCK = 2 * HALF
EPS = 1e-06
CHUNKS = (80, 80, 64, 32)


def parts_of(x):
    high = x.astype(jnp.bfloat16)
    rest = x - high.astype(jnp.float32)
    mid = rest.astype(jnp.bfloat16)
    low = (rest - mid.astype(jnp.float32)).astype(jnp.bfloat16)
    return high, mid, low


def banded(x, band):
    rows = x.shape[0]
    stacked = jnp.concatenate(parts_of(x), axis=0)
    sums = jnp.dot(stacked, band, preferred_element_type=jnp.float32)
    return sums[:rows] + sums[rows:2 * rows] + sums[2 * rows:]


def peer_offsets(peers):
    side = 8 if peers % 8 == 0 else peers
    other = peers // side
    steps = [(dx, dy) for dx in range(other) for dy in range(side) if dx or dy]
    reach = lambda s: min(s[0], other - s[0]) + min(s[1], side - s[1])
    return side, other, sorted(steps, key=reach, reverse=True)


def kernel(
    tm_size, dm_size, widths_in, x, snr, peaks,
    widths, widths_sem, ext, low_band, high_band, low_twice, high_twice, box_band, fm, part, det, split, boxed, rows_max,
    power_out, power_in, scale, col_out, col_in, common, box_common, peak_out, peak_in,
    edge_sem, load_sem, halo_send, halo_recv, head_send, head_recv,
    power_send, power_recv, col_send, col_recv, peak_send, peak_recv, tm_known, dm_known,
):
    rows, length = x.shape
    boxes = widths.shape[0]
    blocks = length // BLOCK
    tiles = length // HALF
    total_len = length * tm_size
    tm = lax.axis_index("tm")
    dm = lax.axis_index("dm")
    right, left = lax.rem(tm + 1, tm_size), lax.rem(tm + tm_size - 1, tm_size)
    side, other, steps = peer_offsets(tm_size)
    tm_x, tm_y = tm // side, tm % side

    def tm_peer(step):
        return lax.rem(tm_x + step[0], other) * side + lax.rem(tm_y + step[1], side)

    dm_steps = sorted(range(1, dm_size), key=lambda d: min(d, dm_size - d), reverse=True)

    spans = [pl.ds(sum(CHUNKS[:q]), CHUNKS[q]) for q in range(len(CHUNKS))]
    edge_loads = []
    for q, span in enumerate(spans):
        for b in (blocks, 1):
            edge_loads.append(
                pltpu.make_async_copy(
                    x.at[span, pl.ds((b - 1) * BLOCK, BLOCK)], ext.at[b, span],
                    edge_sem.at[int(b == 1), q],
                )
            )
            edge_loads[-1].start()

    dm_hub = dm_size - 1
    hub_x, hub_y = other // 2, lax.rem(side // 2 + 1, side)
    tm_hub = hub_x * side + hub_y
    is_first, is_last = tm == 0, tm == tm_size - 1
    near_hub = (tm >= tm_hub - 1) & (tm <= tm_hub + 1)
    barrier = pltpu.get_barrier_semaphore()

    def greet(peer):
        pl.semaphore_signal(barrier, inc=1, device_id=peer, device_id_type=MESH)

    @pl.when(jnp.logical_not(is_first))
    def _():
        greet({"tm": left})

    @pl.when(jnp.logical_not(is_last))
    def _():
        greet({"tm": right})

    @pl.when(jnp.logical_not(near_hub))
    def _():
        greet({"tm": tm_hub})

    @pl.when(dm != dm_hub)
    def _():
        greet({"dm": dm_hub})

    beside = jnp.minimum(tm, 1) + jnp.minimum(tm_size - 1 - tm, 1)
    greetings = jnp.where(tm == tm_hub, tm_size - 1, beside)
    greetings = greetings + jnp.where(dm == dm_hub, dm_size - 1, 0)

    for load in edge_loads[:2]:
        load.wait()
    pl.semaphore_wait(barrier, greetings)
    to_right, to_left = [], []
    for q, span in enumerate(spans):
        to_right.append(
            pltpu.make_async_remote_copy(
                src_ref=ext.at[blocks, span], dst_ref=ext.at[0, span],
                send_sem=halo_send.at[0, q], recv_sem=halo_recv.at[0, q],
                device_id={"tm": right}, device_id_type=MESH,
            )
        )
        to_left.append(
            pltpu.make_async_remote_copy(
                src_ref=ext.at[1, span], dst_ref=ext.at[blocks + 1, span],
                send_sem=halo_send.at[1, q], recv_sem=halo_recv.at[1, q],
                device_id={"tm": left}, device_id_type=MESH,
            )
        )
    for q in range(len(spans)):
        if q > 0:
            edge_loads[2 * q].wait()
            edge_loads[2 * q + 1].wait()

        @pl.when(jnp.logical_not(is_last))
        def _():
            to_right[q].start()

        @pl.when(jnp.logical_not(is_first))
        def _():
            to_left[q].start()

    loads = {}
    for b in range(2, blocks):
        loads[b] = pltpu.make_async_copy(
            x.at[:, pl.ds((b - 1) * BLOCK, BLOCK)], ext.at[b], load_sem.at[b - 1]
        )
        loads[b].start()
    fetch = pltpu.make_async_copy(widths_in, widths, widths_sem)
    fetch.start()

    @pl.when(tm == tm_hub)
    def _():
        for step in steps:
            pl.semaphore_signal(
                tm_known, inc=1, device_id={"tm": tm_peer(step)}, device_id_type=MESH
            )

    @pl.when(dm == dm_hub)
    def _():
        for d in range(dm_size - 1):
            pl.semaphore_signal(dm_known, inc=1, device_id={"dm": d}, device_id_type=MESH)

    row_idx = lax.broadcasted_iota(jnp.int32, (BLOCK, BLOCK), 0)
    col_idx = lax.broadcasted_iota(jnp.int32, (BLOCK, BLOCK), 1)
    low = (row_idx >= col_idx).astype(jnp.float32).astype(jnp.bfloat16)
    high = (row_idx <= col_idx).astype(jnp.float32).astype(jnp.bfloat16)
    low_band[...] = low
    high_band[...] = high
    span_len = (row_idx - col_idx).astype(jnp.float32)
    low_twice[...] = jnp.maximum(span_len + 1.0, 0.0).astype(jnp.bfloat16)
    high_twice[...] = jnp.maximum(1.0 - span_len, 0.0).astype(jnp.bfloat16)

    def inverse_counts(first):
        pos = first + lax.broadcasted_iota(jnp.int32, (1, BLOCK), 1)
        counts = (jnp.minimum(pos + HALF, total_len - 1) - jnp.maximum(pos - HALF, 0) + 1)
        valid = (pos >= 0) & (pos < total_len)
        return jnp.where(valid, 1.0 / jnp.maximum(counts, 1).astype(jnp.float32), 0.0)

    offset = tm * length
    inner = 1.0 / (2 * HALF + 1)
    edge_first = inverse_counts(offset - HALF)
    edge_last = inverse_counts(offset + length - HALF)
    own_first = inverse_counts(offset)
    own_last = inverse_counts(offset + length - BLOCK)

    for b in range(2, blocks):
        loads[b].wait()
    for b in range(1, blocks):
        sums = banded(ext[b], low_band[...]) + banded(ext[b + 1], high_band[...])
        fm[b] = sums * inner
    mean = banded(ext[1], high_band[...]) * edge_first
    smooth = banded(fm[1], high_band[...]) + banded(mean, low_band[...])
    part[0] = ext[1] - smooth * own_first
    mean = banded(ext[blocks], low_band[...]) * edge_last
    smooth = banded(fm[blocks - 1], low_band[...]) + banded(mean, high_band[...])
    part[1] = ext[blocks] - smooth * own_last

    def keep(block_idx, span, values):
        for k, piece in enumerate(parts_of(values)):
            split[k, span, pl.ds(block_idx * BLOCK, BLOCK)] = piece
        det[span, pl.ds(block_idx * BLOCK, BLOCK)] = values
        squares = values * values
        return squares[:, :HALF] + squares[:, HALF:]

    power = jnp.zeros((rows, HALF), jnp.float32)
    for b in range(1, blocks - 1):
        smooth = (banded(fm[b], low_band[...]) + banded(fm[b + 1], high_band[...])) * inner
        power = power + keep(b, pl.ds(0, rows), ext[b + 1] - smooth)
    rows_max[0] = power

    for q, span in enumerate(spans):
        @pl.when(jnp.logical_not(is_first))
        def _():
            to_right[q].wait_recv()

        @pl.when(jnp.logical_not(is_last))
        def _():
            to_left[q].wait_recv()

        before = jnp.where(is_first, 0.0, ext[0, span])
        after = jnp.where(is_last, 0.0, ext[blocks + 1, span])
        from_before = banded(before, low_twice[...]) * (inner * inner)
        from_after = banded(after, high_twice[...]) * (inner * inner)
        power = keep(0, span, part[0, span] - from_before)
        power = power + keep(blocks - 1, span, part[1, span] - from_after)
        rows_max[0, span] = rows_max[0, span] + power

    for h in range(rows // HALF):
        turned = rows_max[0, pl.ds(h * HALF, HALF)].T
        power_out[pl.ds(h, 1), :] = jnp.sum(turned, axis=0, keepdims=True)

    @pl.when(tm != tm_hub)
    def _():
        pl.semaphore_wait(tm_known, 1)

    def to_peers(src, dst, send_sem, recv_sem):
        for step in steps:
            pltpu.make_async_remote_copy(
                src_ref=src, dst_ref=dst.at[step[0] * side + step[1] - 1],
                send_sem=send_sem, recv_sem=recv_sem,
                device_id={"tm": tm_peer(step)}, device_id_type=MESH,
            ).start()

    to_peers(power_out, power_in, power_send, power_recv)
    head = pltpu.make_async_remote_copy(
        src_ref=det.at[:, pl.ds(0, HALF)], dst_ref=det.at[:, pl.ds(length, HALF)],
        send_sem=head_send, recv_sem=head_recv,
        device_id={"tm": left}, device_id_type=MESH,
    )

    @pl.when(jnp.logical_not(is_first))
    def _():
        head.start()


    fetch.wait()
    lane = lax.broadcasted_iota(jnp.int32, (BLOCK, HALF), 1)
    depth = lax.broadcasted_iota(jnp.int32, (BLOCK, HALF), 0)
    for i in range(boxes):
        inside = (depth >= lane) & (depth < lane + widths[i])
        for k in range(3):
            box_band[pl.ds(k * BLOCK, BLOCK), pl.ds(i * HALF, HALF)] = inside.astype(
                jnp.float32
            ).astype(jnp.bfloat16)

    def box_sums(t):
        window = jnp.concatenate(
            [split[k, :, pl.ds(t * HALF, BLOCK)] for k in range(3)], axis=1
        )
        boxed[t] = jnp.dot(window, box_band[...], preferred_element_type=jnp.float32)

    for t in range(tiles - 1):
        box_sums(t)

    @pl.when(dm != dm_hub)
    def _():
        pl.semaphore_wait(dm_known, 1)

    pltpu.make_async_copy(power_in, power_in, power_recv).wait()
    totals = power_out[...] + jnp.sum(power_in[...], axis=0)
    inverse_scale = 1.0 / jnp.sqrt(totals * (1.0 / total_len) + EPS)
    for h in range(rows // HALF):
        row = jnp.broadcast_to(inverse_scale[h:h + 1, :], (HALF, HALF))
        scale[pl.ds(h * HALF, HALF), :] = row.T

    @pl.when(jnp.logical_not(is_last))
    def _():
        head.wait_recv()

    det[:, pl.ds(length, HALF)] = jnp.where(is_last, 0.0, det[:, pl.ds(length, HALF)])
    sums = [jnp.zeros((8, HALF), jnp.float32) for _ in range(tiles + 1)]
    for r in range(rows // 8):
        gain = scale[pl.ds(r * 8, 8), :]
        for t in range(tiles + 1):
            sums[t] = sums[t] + det[pl.ds(r * 8, 8), pl.ds(t * HALF, HALF)] * gain
    for t in range(tiles + 1):
        col_out[pl.ds(t, 1), :] = jnp.sum(sums[t], axis=0, keepdims=True)
    for d in dm_steps:
        pltpu.make_async_remote_copy(
            src_ref=col_out, dst_ref=col_in.at[d - 1], send_sem=col_send, recv_sem=col_recv,
            device_id={"dm": lax.rem(dm + d, dm_size)}, device_id_type=MESH,
        ).start()

    for k, piece in enumerate(parts_of(det[:, pl.ds(length, HALF)])):
        split[k, :, pl.ds(length, HALF)] = piece
    box_sums(tiles - 1)

    inverse = []
    for i in range(boxes):
        width = jnp.full((16, HALF), widths[i], jnp.int32).astype(jnp.float32)
        inverse.append(1.0 / jnp.sqrt(width))

    pltpu.make_async_copy(col_in, col_in, col_recv).wait()
    column_total = col_out[...] + jnp.sum(col_in[...], axis=0)
    common[...] = column_total * (1.0 / (rows * dm_size))
    window = jnp.concatenate([common[pl.ds(0, tiles), :], common[pl.ds(1, tiles), :]], axis=1)
    box_common[...] = banded(window, box_band[pl.ds(0, BLOCK), :])

    for i in range(boxes):
        offsets = [
            jnp.broadcast_to(box_common[pl.ds(t, 1), pl.ds(i * HALF, HALF)], (16, HALF)) * inverse[i]
            for t in range(tiles)
        ]

        def some_rows(r, carry):
            for k in range(4):
                span = pl.ds(pl.multiple_of(r * 64 + k * 16, 16), 16)
                gain = scale[span, :] * inverse[i]
                most = None
                for t in range(tiles):
                    series = boxed[t, span, pl.ds(i * HALF, HALF)] * gain - offsets[t]
                    most = series if most is None else jnp.maximum(most, series)
                    snr[i, span, pl.ds(t * HALF, HALF)] = series.astype(jnp.bfloat16)
                rows_max[i, span] = most
            return carry

        lax.fori_loop(0, rows // 64, some_rows, 0)

    halves = rows // HALF
    for i in range(boxes):
        for h in range(halves):
            turned = rows_max[i, pl.ds(h * HALF, HALF)].T
            peak_out[pl.ds(i * halves + h, 1), :] = jnp.max(turned, axis=0, keepdims=True)
    to_peers(peak_out, peak_in, peak_send, peak_recv)
    pltpu.make_async_copy(peak_in, peak_in, peak_recv).wait()
    most = jnp.maximum(peak_out[...], jnp.max(peak_in[...], axis=0))
    for i in range(boxes):
        for h in range(halves):
            row = i * halves + h
            peaks[pl.ds(i, 1), pl.ds(h * HALF, HALF)] = most[row:row + 1, :]

    @pl.when(jnp.logical_not(is_last))
    def _():
        for copy in to_right:
            copy.wait_send()

    @pl.when(jnp.logical_not(is_first))
    def _():
        for copy in to_left:
            copy.wait_send()
        head.wait_send()

    pltpu.make_async_copy(power_in, power_in, power_send).wait()
    pltpu.make_async_copy(col_in, col_in, col_send).wait()
    pltpu.make_async_copy(peak_in, peak_in, peak_send).wait()


def hand_out(snr, peaks, snr_out, peaks_out, sems):
    boxes = snr.shape[0]
    copies = [pltpu.make_async_copy(peaks, peaks_out, sems.at[boxes])]
    copies += [pltpu.make_async_copy(snr.at[i], snr_out.at[i], sems.at[i]) for i in range(boxes)]
    for copy in copies:
        copy.start()
    for copy in copies:
        copy.wait()


def solution(mesh):
    tm_size, dm_size = mesh.shape["tm"], mesh.shape["dm"]

    def step(dispersed, widths):
        rows, length = dispersed.shape
        boxes = widths.shape[0]
        blocks, tiles, halves = length // BLOCK, length // HALF, rows // HALF
        f32, bf16 = jnp.float32, jnp.bfloat16
        dma = pltpu.SemaphoreType.DMA
        inputs = [pltpu.with_memory_space_constraint(a, pltpu.HBM) for a in (widths, dispersed)]
        snr, peaks = pl.pallas_call(
            functools.partial(kernel, tm_size, dm_size),
            out_shape=(
                pltpu.VMEM((boxes, rows, length), bf16),
                pltpu.VMEM((boxes, rows), f32),
            ),
            in_specs=[pl.BlockSpec(memory_space=pltpu.HBM)] * 2,
            out_specs=(pl.BlockSpec(memory_space=pltpu.VMEM),) * 2,
            scratch_shapes=[
                pltpu.SMEM((boxes,), jnp.int32),
                dma,
                pltpu.VMEM((blocks + 2, rows, BLOCK), f32),
                pltpu.VMEM((BLOCK, BLOCK), bf16),
                pltpu.VMEM((BLOCK, BLOCK), bf16),
                pltpu.VMEM((BLOCK, BLOCK), bf16),
                pltpu.VMEM((BLOCK, BLOCK), bf16),
                pltpu.VMEM((3 * BLOCK, boxes * HALF), bf16),
                pltpu.VMEM((blocks, rows, BLOCK), f32),
                pltpu.VMEM((2, rows, BLOCK), f32),
                pltpu.VMEM((rows, length + HALF), f32),
                pltpu.VMEM((3, rows, length + HALF), bf16),
                pltpu.VMEM((tiles, rows, boxes * HALF), f32),
                pltpu.VMEM((boxes, rows, HALF), f32),
                pltpu.VMEM((halves, HALF), f32),
                pltpu.VMEM((tm_size - 1, halves, HALF), f32),
                pltpu.VMEM((rows, HALF), f32),
                pltpu.VMEM((tiles + 1, HALF), f32),
                pltpu.VMEM((dm_size - 1, tiles + 1, HALF), f32),
                pltpu.VMEM((tiles + 1, HALF), f32),
                pltpu.VMEM((tiles, boxes * HALF), f32),
                pltpu.VMEM((boxes * halves, HALF), f32),
                pltpu.VMEM((tm_size - 1, boxes * halves, HALF), f32),
                dma((2, len(CHUNKS))),
                dma((blocks,)),
                dma((2, len(CHUNKS))),
                dma((2, len(CHUNKS))),
                dma, dma, dma, dma, dma, dma, dma, dma,
                pltpu.SemaphoreType.REGULAR,
                pltpu.SemaphoreType.REGULAR,
            ],
            compiler_params=pltpu.CompilerParams(
                collective_id=0, has_side_effects=True, vmem_limit_bytes=48 * 2**20
            ),
        )(*inputs)
        return pl.pallas_call(
            hand_out,
            out_shape=(
                jax.ShapeDtypeStruct(snr.shape, bf16),
                jax.ShapeDtypeStruct(peaks.shape, f32),
            ),
            in_specs=[pl.BlockSpec(memory_space=pl.ANY)] * 2,
            out_specs=(pl.BlockSpec(memory_space=pl.ANY),) * 2,
            scratch_shapes=[dma((boxes + 1,))],
            compiler_params=pltpu.CompilerParams(vmem_limit_bytes=2**22),
        )(snr, peaks)

    return jax.shard_map(
        step,
        mesh=mesh,
        in_specs=(P("dm", "tm"), P()),
        out_specs=(P(None, "dm", "tm"), P(None, "dm")),
        check_vma=False,
    )
```

```python
import functools

import jax
import jax.numpy as jnp
from jax import lax
from jax.experimental import pallas as pl
from jax.experimental.pallas import tpu as pltpu
from jax.sharding import PartitionSpec as P

MESH = pl.DeviceIdType.MESH
HALF = 128
BLOCK = 2 * HALF
EPS = 1e-06
CHUNKS = (80, 80, 64, 32)


def parts_of(x):
    high = x.astype(jnp.bfloat16)
    rest = x - high.astype(jnp.float32)
    mid = rest.astype(jnp.bfloat16)
    low = (rest - mid.astype(jnp.float32)).astype(jnp.bfloat16)
    return high, mid, low


def banded(x, band):
    rows = x.shape[0]
    stacked = jnp.concatenate(parts_of(x), axis=0)
    sums = jnp.dot(stacked, band, preferred_element_type=jnp.float32)
    return sums[:rows] + sums[rows:2 * rows] + sums[2 * rows:]


def wrapped(index, size):
    return jnp.where(index >= size, index - size, index)


def peer_offsets(peers):
    side = 8 if peers % 8 == 0 else peers
    other = peers // side
    steps = [(dx, dy) for dx in range(other) for dy in range(side) if dx or dy]
    reach = lambda s: min(s[0], other - s[0]) + min(s[1], side - s[1])
    return side, other, sorted(steps, key=reach, reverse=True)


def kernel(
    tm_size, dm_size, widths_in, x, snr, peaks,
    widths, widths_sem, ext, low_band, high_band, low_twice, high_twice, box_band, fm, part, det, split, boxed, acc,
    power_out, power_in, scale, col_out, col_in, common, box_common, peak_out, peak_in,
    edge_sem, load_sem, halo_send, halo_recv, head_send, head_recv,
    power_send, power_recv, col_send, col_recv, peak_send, peak_recv, tm_known, dm_known,
):
    rows, length = x.shape
    boxes = widths.shape[0]
    blocks = length // BLOCK
    tiles = length // HALF
    total_len = length * tm_size
    tm = lax.axis_index("tm")
    dm = lax.axis_index("dm")
    right, left = wrapped(tm + 1, tm_size), wrapped(tm + tm_size - 1, tm_size)
    side, other, steps = peer_offsets(tm_size)
    tm_x = tm // side
    tm_y = tm - tm_x * side

    def tm_peer(step):
        return wrapped(tm_x + step[0], other) * side + wrapped(tm_y + step[1], side)


    spans = [pl.ds(sum(CHUNKS[:q]), CHUNKS[q]) for q in range(len(CHUNKS))]
    edge_loads = []
    for q, span in enumerate(spans):
        for b in (blocks, 1):
            edge_loads.append(
                pltpu.make_async_copy(
                    x.at[span, pl.ds((b - 1) * BLOCK, BLOCK)], ext.at[b, span],
                    edge_sem.at[int(b == 1), q],
                )
            )
            edge_loads[-1].start()

    dm_hub = dm_size - 1
    hub_x, hub_y = other // 2, (side // 2 + 1) % side
    tm_hub = hub_x * side + hub_y
    is_first, is_last = tm == 0, tm == tm_size - 1
    near_hub = (tm >= tm_hub - 1) & (tm <= tm_hub + 1)
    barrier = pltpu.get_barrier_semaphore()

    def greet(peer):
        pl.semaphore_signal(barrier, inc=1, device_id=peer, device_id_type=MESH)

    @pl.when(jnp.logical_not(is_first))
    def _():
        greet({"tm": left})

    @pl.when(jnp.logical_not(is_last))
    def _():
        greet({"tm": right})

    @pl.when(jnp.logical_not(near_hub))
    def _():
        greet({"tm": tm_hub})

    @pl.when(dm != dm_hub)
    def _():
        greet({"dm": dm_hub})

    beside = jnp.minimum(tm, 1) + jnp.minimum(tm_size - 1 - tm, 1)
    greetings = jnp.where(tm == tm_hub, tm_size - 1, beside)
    greetings = greetings + jnp.where(dm == dm_hub, dm_size - 1, 0)

    for load in edge_loads[:2]:
        load.wait()
    pl.semaphore_wait(barrier, greetings)
    to_right, to_left = [], []
    for q, span in enumerate(spans):
        to_right.append(
            pltpu.make_async_remote_copy(
                src_ref=ext.at[blocks, span], dst_ref=ext.at[0, span],
                send_sem=halo_send.at[0, q], recv_sem=halo_recv.at[0, q],
                device_id={"tm": right}, device_id_type=MESH,
            )
        )
        to_left.append(
            pltpu.make_async_remote_copy(
                src_ref=ext.at[1, span], dst_ref=ext.at[blocks + 1, span],
                send_sem=halo_send.at[1, q], recv_sem=halo_recv.at[1, q],
                device_id={"tm": left}, device_id_type=MESH,
            )
        )
    for q in range(len(spans)):
        if q > 0:
            edge_loads[2 * q].wait()
            edge_loads[2 * q + 1].wait()

        @pl.when(jnp.logical_not(is_last))
        def _():
            to_right[q].start()

        @pl.when(jnp.logical_not(is_first))
        def _():
            to_left[q].start()

    loads = {}
    for b in range(2, blocks):
        loads[b] = pltpu.make_async_copy(
            x.at[:, pl.ds((b - 1) * BLOCK, BLOCK)], ext.at[b], load_sem.at[b - 1]
        )
        loads[b].start()
    fetch = pltpu.make_async_copy(widths_in, widths, widths_sem)
    fetch.start()

    @pl.when(tm == tm_hub)
    def _():
        for step in steps:
            pl.semaphore_signal(
                tm_known, inc=1, device_id={"tm": tm_peer(step)}, device_id_type=MESH
            )

    @pl.when(dm == dm_hub)
    def _():
        for d in range(dm_size - 1):
            pl.semaphore_signal(dm_known, inc=1, device_id={"dm": d}, device_id_type=MESH)

    row_idx = lax.broadcasted_iota(jnp.int32, (BLOCK, BLOCK), 0)
    col_idx = lax.broadcasted_iota(jnp.int32, (BLOCK, BLOCK), 1)
    low = (row_idx >= col_idx).astype(jnp.float32).astype(jnp.bfloat16)
    high = (row_idx <= col_idx).astype(jnp.float32).astype(jnp.bfloat16)
    low_band[...] = low
    high_band[...] = high
    span_len = (row_idx - col_idx).astype(jnp.float32)
    low_twice[...] = jnp.maximum(span_len + 1.0, 0.0).astype(jnp.bfloat16)
    high_twice[...] = jnp.maximum(1.0 - span_len, 0.0).astype(jnp.bfloat16)

    def inverse_counts(first):
        pos = first + lax.broadcasted_iota(jnp.int32, (1, BLOCK), 1)
        counts = (jnp.minimum(pos + HALF, total_len - 1) - jnp.maximum(pos - HALF, 0) + 1)
        valid = (pos >= 0) & (pos < total_len)
        return jnp.where(valid, 1.0 / jnp.maximum(counts, 1).astype(jnp.float32), 0.0)

    offset = tm * length
    inner = 1.0 / (2 * HALF + 1)
    edge_first = inverse_counts(offset - HALF)
    edge_last = inverse_counts(offset + length - HALF)
    own_first = inverse_counts(offset)
    own_last = inverse_counts(offset + length - BLOCK)

    for b in range(2, blocks):
        loads[b].wait()
    for b in range(1, blocks):
        sums = banded(ext[b], low_band[...]) + banded(ext[b + 1], high_band[...])
        fm[b] = sums * inner
    mean = banded(ext[1], high_band[...]) * edge_first
    smooth = banded(fm[1], high_band[...]) + banded(mean, low_band[...])
    part[0] = ext[1] - smooth * own_first
    mean = banded(ext[blocks], low_band[...]) * edge_last
    smooth = banded(fm[blocks - 1], low_band[...]) + banded(mean, high_band[...])
    part[1] = ext[blocks] - smooth * own_last

    def keep(block_idx, span, values):
        for k, piece in enumerate(parts_of(values)):
            split[k, span, pl.ds(block_idx * BLOCK, BLOCK)] = piece
        det[span, pl.ds(block_idx * BLOCK, BLOCK)] = values
        squares = values * values
        return squares[:, :HALF] + squares[:, HALF:]

    power = jnp.zeros((rows, HALF), jnp.float32)
    for b in range(1, blocks - 1):
        smooth = (banded(fm[b], low_band[...]) + banded(fm[b + 1], high_band[...])) * inner
        power = power + keep(b, pl.ds(0, rows), ext[b + 1] - smooth)
    acc[...] = power

    for q, span in enumerate(spans):
        @pl.when(jnp.logical_not(is_first))
        def _():
            to_right[q].wait_recv()

        @pl.when(jnp.logical_not(is_last))
        def _():
            to_left[q].wait_recv()

        before = jnp.where(is_first, 0.0, ext[0, span])
        after = jnp.where(is_last, 0.0, ext[blocks + 1, span])
        from_before = banded(before, low_twice[...]) * (inner * inner)
        from_after = banded(after, high_twice[...]) * (inner * inner)
        power = keep(0, span, part[0, span] - from_before)
        power = power + keep(blocks - 1, span, part[1, span] - from_after)
        acc[span, :] = acc[span, :] + power

    for h in range(rows // HALF):
        turned = acc[pl.ds(h * HALF, HALF), :].T
        power_out[pl.ds(h, 1), :] = jnp.sum(turned, axis=0, keepdims=True)

    @pl.when(tm != tm_hub)
    def _():
        pl.semaphore_wait(tm_known, 1)

    late = lambda d, n: 1.5 * min(d, n - d) + (d > n // 2) + 0.5 * (d == n // 2)
    reach = lambda p: (p[0] > 0) + 0.1 * min(p[0], other - p[0]) + late(p[1], side)
    places = sorted(((px, py) for px in range(other) for py in range(side)), key=reach)

    def to_all(src, dst, send_sem, recv_sem, order):
        for px, py in order:
            target = px * side + py
            slot = wrapped(px - tm_x + other, other) * side + wrapped(py - tm_y + side, side) - 1

            @pl.when(tm != target)
            def _():
                pltpu.make_async_remote_copy(
                    src_ref=src, dst_ref=dst.at[slot], send_sem=send_sem, recv_sem=recv_sem,
                    device_id={"tm": target}, device_id_type=MESH,
                ).start()

    to_all(power_out, power_in, power_send, power_recv, places[::-1])
    head = pltpu.make_async_remote_copy(
        src_ref=det.at[:, pl.ds(0, HALF)], dst_ref=det.at[:, pl.ds(length, HALF)],
        send_sem=head_send, recv_sem=head_recv,
        device_id={"tm": left}, device_id_type=MESH,
    )

    @pl.when(jnp.logical_not(is_first))
    def _():
        head.start()


    fetch.wait()
    lane = lax.broadcasted_iota(jnp.int32, (BLOCK, HALF), 1)
    depth = lax.broadcasted_iota(jnp.int32, (BLOCK, HALF), 0)
    for i in range(boxes):
        inside = (depth >= lane) & (depth < lane + widths[i])
        for k in range(3):
            box_band[pl.ds(k * BLOCK, BLOCK), pl.ds(i * HALF, HALF)] = inside.astype(
                jnp.float32
            ).astype(jnp.bfloat16)

    def box_sums(t):
        window = jnp.concatenate(
            [split[k, :, pl.ds(t * HALF, BLOCK)] for k in range(3)], axis=1
        )
        boxed[t] = jnp.dot(window, box_band[...], preferred_element_type=jnp.float32)

    for t in range(tiles - 1):
        box_sums(t)

    @pl.when(dm != dm_hub)
    def _():
        pl.semaphore_wait(dm_known, 1)

    pltpu.make_async_copy(power_in, power_in, power_recv).wait()
    totals = power_out[...] + jnp.sum(power_in[...], axis=0)
    inverse_scale = 1.0 / jnp.sqrt(totals * (1.0 / total_len) + EPS)
    for h in range(rows // HALF):
        row = jnp.broadcast_to(inverse_scale[h:h + 1, :], (HALF, HALF))
        scale[pl.ds(h * HALF, HALF), :] = row.T

    @pl.when(jnp.logical_not(is_last))
    def _():
        head.wait_recv()

    det[:, pl.ds(length, HALF)] = jnp.where(is_last, 0.0, det[:, pl.ds(length, HALF)])
    sums = [jnp.zeros((8, HALF), jnp.float32) for _ in range(tiles + 1)]
    for r in range(rows // 8):
        gain = scale[pl.ds(r * 8, 8), :]
        for t in range(tiles + 1):
            sums[t] = sums[t] + det[pl.ds(r * 8, 8), pl.ds(t * HALF, HALF)] * gain
    for t in range(tiles + 1):
        col_out[pl.ds(t, 1), :] = jnp.sum(sums[t], axis=0, keepdims=True)
    for target in range(dm_size):

        @pl.when(dm != target)
        def _():
            pltpu.make_async_remote_copy(
                src_ref=col_out, dst_ref=col_in.at[wrapped(target - dm + dm_size, dm_size) - 1],
                send_sem=col_send, recv_sem=col_recv,
                device_id={"dm": target}, device_id_type=MESH,
            ).start()

    for k, piece in enumerate(parts_of(det[:, pl.ds(length, HALF)])):
        split[k, :, pl.ds(length, HALF)] = piece
    box_sums(tiles - 1)

    inverse = []
    for i in range(boxes):
        width = jnp.full((8, HALF), widths[i], jnp.int32).astype(jnp.float32)
        inverse.append(1.0 / jnp.sqrt(width))

    def scale_rows(r, carry):
        span = pl.ds(pl.multiple_of(r * 8, 8), 8)
        gain = scale[span, :]
        for i in range(boxes):
            gain_i = gain * inverse[i]
            for t in range(tiles):
                lanes = pl.ds(i * HALF, HALF)
                boxed[t, span, lanes] = boxed[t, span, lanes] * gain_i
        return carry

    lax.fori_loop(0, rows // 8, scale_rows, 0)

    pltpu.make_async_copy(col_in, col_in, col_recv).wait()
    column_total = col_out[...] + jnp.sum(col_in[...], axis=0)
    common[...] = column_total * (1.0 / (rows * dm_size))
    window = jnp.concatenate([common[pl.ds(0, tiles), :], common[pl.ds(1, tiles), :]], axis=1)
    box_common[...] = banded(window, box_band[pl.ds(0, BLOCK), :])

    halves = rows // HALF
    offsets = [
        [
            jnp.broadcast_to(box_common[pl.ds(t, 1), pl.ds(i * HALF, HALF)], (8, HALF)) * inverse[i]
            for t in range(tiles)
        ]
        for i in range(boxes)
    ]

    def series_of(i, t, span):
        return boxed[t, span, pl.ds(i * HALF, HALF)] - offsets[i][t]

    for i in range(boxes):
        for h in range(halves):
            pieces = []
            for r in range(HALF // 8):
                span = pl.ds(h * HALF + r * 8, 8)
                values = [series_of(i, t, span) for t in range(tiles)]
                while len(values) > 1:
                    values = [jnp.maximum(a, b) for a, b in zip(values[::2], values[1::2])]
                pieces.append(values[0])
            turned = jnp.concatenate(pieces, axis=0).T
            peak_out[pl.ds(i * halves + h, 1), :] = jnp.max(turned, axis=0, keepdims=True)
    to_all(peak_out, peak_in, peak_send, peak_recv, places)

    for i in range(boxes):

        def some_rows(r, carry):
            top = pl.ds(pl.multiple_of(r * 16, 16), 8)
            bottom = pl.ds(pl.multiple_of(r * 16 + 8, 8), 8)
            both = pl.ds(pl.multiple_of(r * 16, 16), 16)
            for t in range(tiles):
                pair = jnp.concatenate([series_of(i, t, top), series_of(i, t, bottom)], axis=0)
                snr[i, both, pl.ds(t * HALF, HALF)] = pair.astype(jnp.bfloat16)
            return carry

        lax.fori_loop(0, rows // 16, some_rows, 0)

    pltpu.make_async_copy(peak_in, peak_in, peak_recv).wait()
    most = jnp.maximum(peak_out[...], jnp.max(peak_in[...], axis=0))
    for i in range(boxes):
        for h in range(halves):
            row = i * halves + h
            peaks[pl.ds(i, 1), pl.ds(h * HALF, HALF)] = most[row:row + 1, :]

    @pl.when(jnp.logical_not(is_last))
    def _():
        for copy in to_right:
            copy.wait_send()

    @pl.when(jnp.logical_not(is_first))
    def _():
        for copy in to_left:
            copy.wait_send()
        head.wait_send()

    pltpu.make_async_copy(power_in, power_in, power_send).wait()
    pltpu.make_async_copy(col_in, col_in, col_send).wait()
    pltpu.make_async_copy(peak_in, peak_in, peak_send).wait()


def hand_out(snr, peaks, snr_out, peaks_out, peaks_sem, sems):
    boxes, pieces = sems.shape
    rows = snr.shape[1] // pieces
    copies = [pltpu.make_async_copy(peaks, peaks_out, peaks_sem)]
    for i in range(boxes):
        for k in range(pieces):
            span = pl.ds(k * rows, rows)
            copies.append(pltpu.make_async_copy(snr.at[i, span], snr_out.at[i, span], sems.at[i, k]))
    for copy in copies:
        copy.start()
    for copy in copies:
        copy.wait()


def solution(mesh):
    tm_size, dm_size = mesh.shape["tm"], mesh.shape["dm"]

    def step(dispersed, widths):
        rows, length = dispersed.shape
        boxes = widths.shape[0]
        blocks, tiles, halves = length // BLOCK, length // HALF, rows // HALF
        f32, bf16 = jnp.float32, jnp.bfloat16
        dma = pltpu.SemaphoreType.DMA
        inputs = [pltpu.with_memory_space_constraint(a, pltpu.HBM) for a in (widths, dispersed)]
        snr, peaks = pl.pallas_call(
            functools.partial(kernel, tm_size, dm_size),
            out_shape=(
                pltpu.VMEM((boxes, rows, length), bf16),
                pltpu.VMEM((boxes, rows), f32),
            ),
            in_specs=[pl.BlockSpec(memory_space=pltpu.HBM)] * 2,
            out_specs=(pl.BlockSpec(memory_space=pltpu.VMEM),) * 2,
            scratch_shapes=[
                pltpu.SMEM((boxes,), jnp.int32),
                dma,
                pltpu.VMEM((blocks + 2, rows, BLOCK), f32),
                pltpu.VMEM((BLOCK, BLOCK), bf16),
                pltpu.VMEM((BLOCK, BLOCK), bf16),
                pltpu.VMEM((BLOCK, BLOCK), bf16),
                pltpu.VMEM((BLOCK, BLOCK), bf16),
                pltpu.VMEM((3 * BLOCK, boxes * HALF), bf16),
                pltpu.VMEM((blocks, rows, BLOCK), f32),
                pltpu.VMEM((2, rows, BLOCK), f32),
                pltpu.VMEM((rows, length + HALF), f32),
                pltpu.VMEM((3, rows, length + HALF), bf16),
                pltpu.VMEM((tiles, rows, boxes * HALF), f32),
                pltpu.VMEM((rows, HALF), f32),
                pltpu.VMEM((halves, HALF), f32),
                pltpu.VMEM((tm_size - 1, halves, HALF), f32),
                pltpu.VMEM((rows, HALF), f32),
                pltpu.VMEM((tiles + 1, HALF), f32),
                pltpu.VMEM((dm_size - 1, tiles + 1, HALF), f32),
                pltpu.VMEM((tiles + 1, HALF), f32),
                pltpu.VMEM((tiles, boxes * HALF), f32),
                pltpu.VMEM((boxes * halves, HALF), f32),
                pltpu.VMEM((tm_size - 1, boxes * halves, HALF), f32),
                dma((2, len(CHUNKS))),
                dma((blocks,)),
                dma((2, len(CHUNKS))),
                dma((2, len(CHUNKS))),
                dma, dma, dma, dma, dma, dma, dma, dma,
                pltpu.SemaphoreType.REGULAR,
                pltpu.SemaphoreType.REGULAR,
            ],
            compiler_params=pltpu.CompilerParams(
                collective_id=0, has_side_effects=True, vmem_limit_bytes=48 * 2**20
            ),
        )(*inputs)
        return pl.pallas_call(
            hand_out,
            out_shape=(
                jax.ShapeDtypeStruct(snr.shape, bf16),
                jax.ShapeDtypeStruct(peaks.shape, f32),
            ),
            in_specs=[pl.BlockSpec(memory_space=pl.ANY)] * 2,
            out_specs=(pl.BlockSpec(memory_space=pl.ANY),) * 2,
            scratch_shapes=[dma, dma((boxes, 1))],
            compiler_params=pltpu.CompilerParams(vmem_limit_bytes=2**22),
        )(snr, peaks)

    return jax.shard_map(
        step,
        mesh=mesh,
        in_specs=(P("dm", "tm"), P()),
        out_specs=(P(None, "dm", "tm"), P(None, "dm")),
        check_vma=False,
    )
```

```python
import functools

import jax
import jax.numpy as jnp
from jax import lax
from jax.experimental import pallas as pl
from jax.experimental.pallas import tpu as pltpu
from jax.sharding import PartitionSpec as P

MESH = pl.DeviceIdType.MESH
HALF = 128
BLOCK = 2 * HALF
EPS = 1e-06
CHUNKS = (80, 80, 64, 32)


def parts_of(x):
    high = x.astype(jnp.bfloat16)
    rest = x - high.astype(jnp.float32)
    mid = rest.astype(jnp.bfloat16)
    low = (rest - mid.astype(jnp.float32)).astype(jnp.bfloat16)
    return high, mid, low


def banded(x, band):
    rows = x.shape[0]
    stacked = jnp.concatenate(parts_of(x), axis=0)
    sums = jnp.dot(stacked, band, preferred_element_type=jnp.float32)
    return sums[:rows] + sums[rows:2 * rows] + sums[2 * rows:]


def wrapped(index, size):
    return jnp.where(index >= size, index - size, index)


def peer_offsets(peers):
    side = 8 if peers % 8 == 0 else peers
    other = peers // side
    steps = [(dx, dy) for dx in range(other) for dy in range(side) if dx or dy]
    reach = lambda s: min(s[0], other - s[0]) + min(s[1], side - s[1])
    return side, other, sorted(steps, key=reach, reverse=True)


def kernel(
    tm_size, dm_size, widths_in, x, snr, peaks,
    widths, widths_sem, ext, low_band, high_band, low_twice, high_twice, box_band, fm, part, det, split, boxed, acc,
    power_out, power_in, scale, col_out, col_in, common, box_common, peak_out, peak_in,
    edge_sem, load_sem, halo_send, halo_recv, head_send, head_recv,
    power_send, power_recv, col_send, col_recv, peak_send, peak_recv, tm_known, dm_known,
):
    rows, length = x.shape
    boxes = widths.shape[0]
    blocks = length // BLOCK
    tiles = length // HALF
    total_len = length * tm_size
    tm = lax.axis_index("tm")
    dm = lax.axis_index("dm")
    right, left = wrapped(tm + 1, tm_size), wrapped(tm + tm_size - 1, tm_size)
    side, other, steps = peer_offsets(tm_size)
    tm_x = tm // side
    tm_y = tm - tm_x * side

    def tm_peer(step):
        return wrapped(tm_x + step[0], other) * side + wrapped(tm_y + step[1], side)


    spans = [pl.ds(sum(CHUNKS[:q]), CHUNKS[q]) for q in range(len(CHUNKS))]
    edge_loads = []
    for q, span in enumerate(spans):
        for b in (blocks, 1):
            edge_loads.append(
                pltpu.make_async_copy(
                    x.at[span, pl.ds((b - 1) * BLOCK, BLOCK)], ext.at[b, span],
                    edge_sem.at[int(b == 1), q],
                )
            )
            edge_loads[-1].start()

    dm_hub = dm_size - 1
    hub_x, hub_y = other // 2, (side // 2 + 1) % side
    tm_hub = hub_x * side + hub_y
    is_first, is_last = tm == 0, tm == tm_size - 1
    near_hub = (tm >= tm_hub - 1) & (tm <= tm_hub + 1)
    barrier = pltpu.get_barrier_semaphore()

    def greet(peer):
        pl.semaphore_signal(barrier, inc=1, device_id=peer, device_id_type=MESH)

    @pl.when(jnp.logical_not(is_first))
    def _():
        greet({"tm": left})

    @pl.when(jnp.logical_not(is_last))
    def _():
        greet({"tm": right})

    @pl.when(jnp.logical_not(near_hub))
    def _():
        greet({"tm": tm_hub})

    @pl.when(dm != dm_hub)
    def _():
        greet({"dm": dm_hub})

    beside = jnp.minimum(tm, 1) + jnp.minimum(tm_size - 1 - tm, 1)
    greetings = jnp.where(tm == tm_hub, tm_size - 1, beside)
    greetings = greetings + jnp.where(dm == dm_hub, dm_size - 1, 0)

    for load in edge_loads[:2]:
        load.wait()
    pl.semaphore_wait(barrier, greetings)
    to_right, to_left = [], []
    for q, span in enumerate(spans):
        to_right.append(
            pltpu.make_async_remote_copy(
                src_ref=ext.at[blocks, span], dst_ref=ext.at[0, span],
                send_sem=halo_send.at[0, q], recv_sem=halo_recv.at[0, q],
                device_id={"tm": right}, device_id_type=MESH,
            )
        )
        to_left.append(
            pltpu.make_async_remote_copy(
                src_ref=ext.at[1, span], dst_ref=ext.at[blocks + 1, span],
                send_sem=halo_send.at[1, q], recv_sem=halo_recv.at[1, q],
                device_id={"tm": left}, device_id_type=MESH,
            )
        )
    for q in range(len(spans)):
        if q > 0:
            edge_loads[2 * q].wait()
            edge_loads[2 * q + 1].wait()

        @pl.when(jnp.logical_not(is_last))
        def _():
            to_right[q].start()

        @pl.when(jnp.logical_not(is_first))
        def _():
            to_left[q].start()

    loads = {}
    for b in range(2, blocks):
        loads[b] = pltpu.make_async_copy(
            x.at[:, pl.ds((b - 1) * BLOCK, BLOCK)], ext.at[b], load_sem.at[b - 1]
        )
        loads[b].start()
    fetch = pltpu.make_async_copy(widths_in, widths, widths_sem)
    fetch.start()

    @pl.when(tm == tm_hub)
    def _():
        for step in steps:
            pl.semaphore_signal(
                tm_known, inc=1, device_id={"tm": tm_peer(step)}, device_id_type=MESH
            )

    @pl.when(dm == dm_hub)
    def _():
        for d in range(dm_size - 1):
            pl.semaphore_signal(dm_known, inc=1, device_id={"dm": d}, device_id_type=MESH)

    row_idx = lax.broadcasted_iota(jnp.int32, (BLOCK, BLOCK), 0)
    col_idx = lax.broadcasted_iota(jnp.int32, (BLOCK, BLOCK), 1)
    low = (row_idx >= col_idx).astype(jnp.float32).astype(jnp.bfloat16)
    high = (row_idx <= col_idx).astype(jnp.float32).astype(jnp.bfloat16)
    low_band[...] = low
    high_band[...] = high
    span_len = (row_idx - col_idx).astype(jnp.float32)
    low_twice[...] = jnp.maximum(span_len + 1.0, 0.0).astype(jnp.bfloat16)
    high_twice[...] = jnp.maximum(1.0 - span_len, 0.0).astype(jnp.bfloat16)

    def inverse_counts(first):
        pos = first + lax.broadcasted_iota(jnp.int32, (1, BLOCK), 1)
        counts = (jnp.minimum(pos + HALF, total_len - 1) - jnp.maximum(pos - HALF, 0) + 1)
        valid = (pos >= 0) & (pos < total_len)
        return jnp.where(valid, 1.0 / jnp.maximum(counts, 1).astype(jnp.float32), 0.0)

    offset = tm * length
    inner = 1.0 / (2 * HALF + 1)
    edge_first = inverse_counts(offset - HALF)
    edge_last = inverse_counts(offset + length - HALF)
    own_first = inverse_counts(offset)
    own_last = inverse_counts(offset + length - BLOCK)

    for b in range(2, blocks):
        loads[b].wait()
    for b in range(1, blocks):
        sums = banded(ext[b], low_band[...]) + banded(ext[b + 1], high_band[...])
        fm[b] = sums * inner
    mean = banded(ext[1], high_band[...]) * edge_first
    smooth = banded(fm[1], high_band[...]) + banded(mean, low_band[...])
    part[0] = ext[1] - smooth * own_first
    mean = banded(ext[blocks], low_band[...]) * edge_last
    smooth = banded(fm[blocks - 1], low_band[...]) + banded(mean, high_band[...])
    part[1] = ext[blocks] - smooth * own_last

    def keep(block_idx, span, values):
        for k, piece in enumerate(parts_of(values)):
            split[k, span, pl.ds(block_idx * BLOCK, BLOCK)] = piece
        det[span, pl.ds(block_idx * BLOCK, BLOCK)] = values
        squares = values * values
        return squares[:, :HALF] + squares[:, HALF:]

    power = jnp.zeros((rows, HALF), jnp.float32)
    for b in range(1, blocks - 1):
        smooth = (banded(fm[b], low_band[...]) + banded(fm[b + 1], high_band[...])) * inner
        power = power + keep(b, pl.ds(0, rows), ext[b + 1] - smooth)
    acc[...] = power

    for q, span in enumerate(spans):
        @pl.when(jnp.logical_not(is_first))
        def _():
            to_right[q].wait_recv()

        @pl.when(jnp.logical_not(is_last))
        def _():
            to_left[q].wait_recv()

        before = jnp.where(is_first, 0.0, ext[0, span])
        after = jnp.where(is_last, 0.0, ext[blocks + 1, span])
        from_before = banded(before, low_twice[...]) * (inner * inner)
        from_after = banded(after, high_twice[...]) * (inner * inner)
        power = keep(0, span, part[0, span] - from_before)
        power = power + keep(blocks - 1, span, part[1, span] - from_after)
        acc[span, :] = acc[span, :] + power

    for h in range(rows // HALF):
        turned = acc[pl.ds(h * HALF, HALF), :].T
        power_out[pl.ds(h, 1), :] = jnp.sum(turned, axis=0, keepdims=True)

    @pl.when(tm != tm_hub)
    def _():
        pl.semaphore_wait(tm_known, 1)

    late = lambda d, n: 1.5 * min(d, n - d) + (d > n // 2) + 0.5 * (d == n // 2)
    reach = lambda p: (p[0] > 0) + 0.1 * min(p[0], other - p[0]) + late(p[1], side)
    places = sorted(((px, py) for px in range(other) for py in range(side)), key=reach)

    def to_all(src, dst, send_sem, recv_sem, order):
        for px, py in order:
            target = px * side + py
            slot = wrapped(px - tm_x + other, other) * side + wrapped(py - tm_y + side, side) - 1

            @pl.when(tm != target)
            def _():
                pltpu.make_async_remote_copy(
                    src_ref=src, dst_ref=dst.at[slot], send_sem=send_sem, recv_sem=recv_sem,
                    device_id={"tm": target}, device_id_type=MESH,
                ).start()

    to_all(power_out, power_in, power_send, power_recv, places[::-1])
    head = pltpu.make_async_remote_copy(
        src_ref=det.at[:, pl.ds(0, HALF)], dst_ref=det.at[:, pl.ds(length, HALF)],
        send_sem=head_send, recv_sem=head_recv,
        device_id={"tm": left}, device_id_type=MESH,
    )

    @pl.when(jnp.logical_not(is_first))
    def _():
        head.start()


    fetch.wait()
    lane = lax.broadcasted_iota(jnp.int32, (BLOCK, HALF), 1)
    depth = lax.broadcasted_iota(jnp.int32, (BLOCK, HALF), 0)
    for i in range(boxes):
        inside = (depth >= lane) & (depth < lane + widths[i])
        for k in range(3):
            box_band[pl.ds(k * BLOCK, BLOCK), pl.ds(i * HALF, HALF)] = inside.astype(
                jnp.float32
            ).astype(jnp.bfloat16)

    def lanes_of(i, t):
        return pl.ds((i * tiles + t) * HALF, HALF)

    def box_sums(t):
        window = jnp.concatenate(
            [split[k, :, pl.ds(t * HALF, BLOCK)] for k in range(3)], axis=1
        )
        sums = jnp.dot(window, box_band[...], preferred_element_type=jnp.float32)
        for i in range(boxes):
            boxed[:, lanes_of(i, t)] = sums[:, i * HALF:(i + 1) * HALF]

    for t in range(tiles - 1):
        box_sums(t)

    @pl.when(dm != dm_hub)
    def _():
        pl.semaphore_wait(dm_known, 1)

    pltpu.make_async_copy(power_in, power_in, power_recv).wait()
    totals = power_out[...] + jnp.sum(power_in[...], axis=0)
    inverse_scale = 1.0 / jnp.sqrt(totals * (1.0 / total_len) + EPS)
    for h in range(rows // HALF):
        row = jnp.broadcast_to(inverse_scale[h:h + 1, :], (HALF, HALF))
        scale[pl.ds(h * HALF, HALF), :] = row.T

    @pl.when(jnp.logical_not(is_last))
    def _():
        head.wait_recv()

    det[:, pl.ds(length, HALF)] = jnp.where(is_last, 0.0, det[:, pl.ds(length, HALF)])
    sums = [jnp.zeros((8, HALF), jnp.float32) for _ in range(tiles + 1)]
    for r in range(rows // 8):
        gain = scale[pl.ds(r * 8, 8), :]
        for t in range(tiles + 1):
            sums[t] = sums[t] + det[pl.ds(r * 8, 8), pl.ds(t * HALF, HALF)] * gain
    for t in range(tiles + 1):
        col_out[pl.ds(t, 1), :] = jnp.sum(sums[t], axis=0, keepdims=True)
    for target in range(dm_size):

        @pl.when(dm != target)
        def _():
            pltpu.make_async_remote_copy(
                src_ref=col_out, dst_ref=col_in.at[wrapped(target - dm + dm_size, dm_size) - 1],
                send_sem=col_send, recv_sem=col_recv,
                device_id={"dm": target}, device_id_type=MESH,
            ).start()

    for k, piece in enumerate(parts_of(det[:, pl.ds(length, HALF)])):
        split[k, :, pl.ds(length, HALF)] = piece
    box_sums(tiles - 1)

    inverse = []
    for i in range(boxes):
        width = jnp.full((8, HALF), widths[i], jnp.int32).astype(jnp.float32)
        inverse.append(1.0 / jnp.sqrt(width))

    def scale_rows(r, carry):
        span = pl.ds(pl.multiple_of(r * 8, 8), 8)
        gain = scale[span, :]
        for i in range(boxes):
            gain_i = gain * inverse[i]
            for t in range(tiles):
                boxed[span, lanes_of(i, t)] = boxed[span, lanes_of(i, t)] * gain_i
        return carry

    lax.fori_loop(0, rows // 8, scale_rows, 0)

    pltpu.make_async_copy(col_in, col_in, col_recv).wait()
    column_total = col_out[...] + jnp.sum(col_in[...], axis=0)
    common[...] = column_total * (1.0 / (rows * dm_size))
    window = jnp.concatenate([common[pl.ds(0, tiles), :], common[pl.ds(1, tiles), :]], axis=1)
    box_common[...] = banded(window, box_band[pl.ds(0, BLOCK), :])

    halves = rows // HALF
    offsets = [
        [
            jnp.broadcast_to(box_common[pl.ds(t, 1), pl.ds(i * HALF, HALF)], (8, HALF)) * inverse[i]
            for t in range(tiles)
        ]
        for i in range(boxes)
    ]

    def series_of(i, t, span):
        return boxed[span, lanes_of(i, t)] - offsets[i][t]

    for i in range(boxes):
        for h in range(halves):
            pieces = []
            for r in range(HALF // 8):
                span = pl.ds(h * HALF + r * 8, 8)
                values = [series_of(i, t, span) for t in range(tiles)]
                while len(values) > 1:
                    values = [jnp.maximum(a, b) for a, b in zip(values[::2], values[1::2])]
                pieces.append(values[0])
            turned = jnp.concatenate(pieces, axis=0).T
            peak_out[pl.ds(i * halves + h, 1), :] = jnp.max(turned, axis=0, keepdims=True)
    to_all(peak_out, peak_in, peak_send, peak_recv, places)

    for i in range(boxes):

        def some_rows(r, carry):
            top = pl.ds(pl.multiple_of(r * 16, 16), 8)
            bottom = pl.ds(pl.multiple_of(r * 16 + 8, 8), 8)
            both = pl.ds(pl.multiple_of(r * 16, 16), 16)
            for t in range(tiles):
                pair = jnp.concatenate([series_of(i, t, top), series_of(i, t, bottom)], axis=0)
                snr[i, both, pl.ds(t * HALF, HALF)] = pair.astype(jnp.bfloat16)
            return carry

        lax.fori_loop(0, rows // 16, some_rows, 0)

    pltpu.make_async_copy(peak_in, peak_in, peak_recv).wait()
    most = jnp.maximum(peak_out[...], jnp.max(peak_in[...], axis=0))
    for i in range(boxes):
        for h in range(halves):
            row = i * halves + h
            peaks[pl.ds(i, 1), pl.ds(h * HALF, HALF)] = most[row:row + 1, :]

    @pl.when(jnp.logical_not(is_last))
    def _():
        for copy in to_right:
            copy.wait_send()

    @pl.when(jnp.logical_not(is_first))
    def _():
        for copy in to_left:
            copy.wait_send()
        head.wait_send()

    pltpu.make_async_copy(power_in, power_in, power_send).wait()
    pltpu.make_async_copy(col_in, col_in, col_send).wait()
    pltpu.make_async_copy(peak_in, peak_in, peak_send).wait()


def hand_out(snr, peaks, snr_out, peaks_out, peaks_sem, sems):
    boxes, pieces = sems.shape
    rows = snr.shape[1] // pieces
    copies = [pltpu.make_async_copy(peaks, peaks_out, peaks_sem)]
    for i in range(boxes):
        for k in range(pieces):
            span = pl.ds(k * rows, rows)
            copies.append(pltpu.make_async_copy(snr.at[i, span], snr_out.at[i, span], sems.at[i, k]))
    for copy in copies:
        copy.start()
    for copy in copies:
        copy.wait()


def solution(mesh):
    tm_size, dm_size = mesh.shape["tm"], mesh.shape["dm"]

    def step(dispersed, widths):
        rows, length = dispersed.shape
        boxes = widths.shape[0]
        blocks, tiles, halves = length // BLOCK, length // HALF, rows // HALF
        f32, bf16 = jnp.float32, jnp.bfloat16
        dma = pltpu.SemaphoreType.DMA
        inputs = [pltpu.with_memory_space_constraint(a, pltpu.HBM) for a in (widths, dispersed)]
        snr, peaks = pl.pallas_call(
            functools.partial(kernel, tm_size, dm_size),
            out_shape=(
                pltpu.VMEM((boxes, rows, length), bf16),
                pltpu.VMEM((boxes, rows), f32),
            ),
            in_specs=[pl.BlockSpec(memory_space=pltpu.HBM)] * 2,
            out_specs=(pl.BlockSpec(memory_space=pltpu.VMEM),) * 2,
            scratch_shapes=[
                pltpu.SMEM((boxes,), jnp.int32),
                dma,
                pltpu.VMEM((blocks + 2, rows, BLOCK), f32),
                pltpu.VMEM((BLOCK, BLOCK), bf16),
                pltpu.VMEM((BLOCK, BLOCK), bf16),
                pltpu.VMEM((BLOCK, BLOCK), bf16),
                pltpu.VMEM((BLOCK, BLOCK), bf16),
                pltpu.VMEM((3 * BLOCK, boxes * HALF), bf16),
                pltpu.VMEM((blocks, rows, BLOCK), f32),
                pltpu.VMEM((2, rows, BLOCK), f32),
                pltpu.VMEM((rows, length + HALF), f32),
                pltpu.VMEM((3, rows, length + HALF), bf16),
                pltpu.VMEM((rows, boxes * tiles * HALF), f32),
                pltpu.VMEM((rows, HALF), f32),
                pltpu.VMEM((halves, HALF), f32),
                pltpu.VMEM((tm_size - 1, halves, HALF), f32),
                pltpu.VMEM((rows, HALF), f32),
                pltpu.VMEM((tiles + 1, HALF), f32),
                pltpu.VMEM((dm_size - 1, tiles + 1, HALF), f32),
                pltpu.VMEM((tiles + 1, HALF), f32),
                pltpu.VMEM((tiles, boxes * HALF), f32),
                pltpu.VMEM((boxes * halves, HALF), f32),
                pltpu.VMEM((tm_size - 1, boxes * halves, HALF), f32),
                dma((2, len(CHUNKS))),
                dma((blocks,)),
                dma((2, len(CHUNKS))),
                dma((2, len(CHUNKS))),
                dma, dma, dma, dma, dma, dma, dma, dma,
                pltpu.SemaphoreType.REGULAR,
                pltpu.SemaphoreType.REGULAR,
            ],
            compiler_params=pltpu.CompilerParams(
                collective_id=0, has_side_effects=True, vmem_limit_bytes=48 * 2**20
            ),
        )(*inputs)
        return pl.pallas_call(
            hand_out,
            out_shape=(
                jax.ShapeDtypeStruct(snr.shape, bf16),
                jax.ShapeDtypeStruct(peaks.shape, f32),
            ),
            in_specs=[pl.BlockSpec(memory_space=pl.ANY)] * 2,
            out_specs=(pl.BlockSpec(memory_space=pl.ANY),) * 2,
            scratch_shapes=[dma, dma((boxes, 1))],
            compiler_params=pltpu.CompilerParams(vmem_limit_bytes=2**22),
        )(snr, peaks)

    return jax.shard_map(
        step,
        mesh=mesh,
        in_specs=(P("dm", "tm"), P()),
        out_specs=(P(None, "dm", "tm"), P(None, "dm")),
        check_vma=False,
    )
```

```python
import functools

import jax
import jax.numpy as jnp
from jax import lax
from jax.experimental import pallas as pl
from jax.experimental.pallas import tpu as pltpu
from jax.sharding import PartitionSpec as P

MESH = pl.DeviceIdType.MESH
HALF = 128
BLOCK = 2 * HALF
EPS = 1e-06
CHUNKS = (96, 96, 48, 16)


def parts_of(x):
    high = x.astype(jnp.bfloat16)
    rest = x - high.astype(jnp.float32)
    mid = rest.astype(jnp.bfloat16)
    low = (rest - mid.astype(jnp.float32)).astype(jnp.bfloat16)
    return high, mid, low


def banded(x, band):
    rows = x.shape[0]
    stacked = jnp.concatenate(parts_of(x), axis=0)
    sums = jnp.dot(stacked, band, preferred_element_type=jnp.float32)
    return sums[:rows] + sums[rows:2 * rows] + sums[2 * rows:]


def wrapped(index, size):
    return jnp.where(index >= size, index - size, index)


def peer_offsets(peers):
    side = 8 if peers % 8 == 0 else peers
    other = peers // side
    steps = [(dx, dy) for dx in range(other) for dy in range(side) if dx or dy]
    reach = lambda s: min(s[0], other - s[0]) + min(s[1], side - s[1])
    return side, other, sorted(steps, key=reach, reverse=True)


def kernel(
    tm_size, dm_size, widths_in, x, snr, peaks,
    widths, widths_sem, ext, low_band, high_band, low_twice, high_twice, box_band, fm, part, det, split, boxed, acc,
    power_out, power_in, scale, col_out, col_in, common, box_common, peak_out, peak_in,
    edge_sem, load_sem, halo_send, halo_recv, head_send, head_recv,
    power_send, power_recv, col_send, col_recv, peak_send, peak_recv, tm_known, dm_known,
):
    rows, length = x.shape
    boxes = widths.shape[0]
    blocks = length // BLOCK
    tiles = length // HALF
    total_len = length * tm_size
    tm = lax.axis_index("tm")
    dm = lax.axis_index("dm")
    right, left = wrapped(tm + 1, tm_size), wrapped(tm + tm_size - 1, tm_size)
    side, other, steps = peer_offsets(tm_size)
    tm_x = tm // side
    tm_y = tm - tm_x * side

    def tm_peer(step):
        return wrapped(tm_x + step[0], other) * side + wrapped(tm_y + step[1], side)


    dm_hub = dm_size - 1
    hub_x, hub_y = other // 2, (side // 2 + 1) % side
    tm_hub = hub_x * side + hub_y
    is_first, is_last = tm == 0, tm == tm_size - 1
    near_hub = (tm >= tm_hub - 1) & (tm <= tm_hub + 1)
    barrier = pltpu.get_barrier_semaphore()

    def greet(peer):
        pl.semaphore_signal(barrier, inc=1, device_id=peer, device_id_type=MESH)

    @pl.when(jnp.logical_not(is_first))
    def _():
        greet({"tm": left})

    @pl.when(jnp.logical_not(is_last))
    def _():
        greet({"tm": right})

    @pl.when(jnp.logical_not(near_hub))
    def _():
        greet({"tm": tm_hub})

    @pl.when(dm != dm_hub)
    def _():
        greet({"dm": dm_hub})

    spans = [pl.ds(sum(CHUNKS[:q]), CHUNKS[q]) for q in range(len(CHUNKS))]
    edge_loads = []
    for q, span in enumerate(spans):
        for b in (blocks, 1):
            edge_loads.append(
                pltpu.make_async_copy(
                    x.at[span, pl.ds((b - 1) * BLOCK, BLOCK)], ext.at[b, span],
                    edge_sem.at[int(b == 1), q],
                )
            )
            edge_loads[-1].start()

    beside = jnp.minimum(tm, 1) + jnp.minimum(tm_size - 1 - tm, 1)
    greetings = jnp.where(tm == tm_hub, tm_size - 1, beside)
    greetings = greetings + jnp.where(dm == dm_hub, dm_size - 1, 0)

    for load in edge_loads[:2]:
        load.wait()
    pl.semaphore_wait(barrier, greetings)
    to_right, to_left = [], []
    for q, span in enumerate(spans):
        to_right.append(
            pltpu.make_async_remote_copy(
                src_ref=ext.at[blocks, span], dst_ref=ext.at[0, span],
                send_sem=halo_send.at[0, q], recv_sem=halo_recv.at[0, q],
                device_id={"tm": right}, device_id_type=MESH,
            )
        )
        to_left.append(
            pltpu.make_async_remote_copy(
                src_ref=ext.at[1, span], dst_ref=ext.at[blocks + 1, span],
                send_sem=halo_send.at[1, q], recv_sem=halo_recv.at[1, q],
                device_id={"tm": left}, device_id_type=MESH,
            )
        )
    for q in range(len(spans)):
        if q > 0:
            edge_loads[2 * q].wait()
            edge_loads[2 * q + 1].wait()

        @pl.when(jnp.logical_not(is_last))
        def _():
            to_right[q].start()

        @pl.when(jnp.logical_not(is_first))
        def _():
            to_left[q].start()

    loads = {}
    for b in range(2, blocks):
        loads[b] = pltpu.make_async_copy(
            x.at[:, pl.ds((b - 1) * BLOCK, BLOCK)], ext.at[b], load_sem.at[b - 1]
        )
        loads[b].start()
    fetch = pltpu.make_async_copy(widths_in, widths, widths_sem)
    fetch.start()

    @pl.when(tm == tm_hub)
    def _():
        for step in steps:
            pl.semaphore_signal(
                tm_known, inc=1, device_id={"tm": tm_peer(step)}, device_id_type=MESH
            )

    @pl.when(dm == dm_hub)
    def _():
        for d in range(dm_size - 1):
            pl.semaphore_signal(dm_known, inc=1, device_id={"dm": d}, device_id_type=MESH)

    row_idx = lax.broadcasted_iota(jnp.int32, (BLOCK, BLOCK), 0)
    col_idx = lax.broadcasted_iota(jnp.int32, (BLOCK, BLOCK), 1)
    low = (row_idx >= col_idx).astype(jnp.float32).astype(jnp.bfloat16)
    high = (row_idx <= col_idx).astype(jnp.float32).astype(jnp.bfloat16)
    low_band[...] = low
    high_band[...] = high
    span_len = (row_idx - col_idx).astype(jnp.float32)
    low_twice[...] = jnp.maximum(span_len + 1.0, 0.0).astype(jnp.bfloat16)
    high_twice[...] = jnp.maximum(1.0 - span_len, 0.0).astype(jnp.bfloat16)

    def inverse_counts(first):
        pos = first + lax.broadcasted_iota(jnp.int32, (1, BLOCK), 1)
        counts = (jnp.minimum(pos + HALF, total_len - 1) - jnp.maximum(pos - HALF, 0) + 1)
        valid = (pos >= 0) & (pos < total_len)
        return jnp.where(valid, 1.0 / jnp.maximum(counts, 1).astype(jnp.float32), 0.0)

    offset = tm * length
    inner = 1.0 / (2 * HALF + 1)
    edge_first = inverse_counts(offset - HALF)
    edge_last = inverse_counts(offset + length - HALF)
    own_first = inverse_counts(offset)
    own_last = inverse_counts(offset + length - BLOCK)

    for b in range(2, blocks):
        loads[b].wait()
    for b in range(1, blocks):
        sums = banded(ext[b], low_band[...]) + banded(ext[b + 1], high_band[...])
        fm[b] = sums * inner
    mean = banded(ext[1], high_band[...]) * edge_first
    smooth = banded(fm[1], high_band[...]) + banded(mean, low_band[...])
    part[0] = ext[1] - smooth * own_first
    mean = banded(ext[blocks], low_band[...]) * edge_last
    smooth = banded(fm[blocks - 1], low_band[...]) + banded(mean, high_band[...])
    part[1] = ext[blocks] - smooth * own_last

    def keep(block_idx, span, values):
        det[span, pl.ds(block_idx * BLOCK, BLOCK)] = values
        squares = values * values
        return squares[:, :HALF] + squares[:, HALF:]

    power = jnp.zeros((rows, HALF), jnp.float32)
    for b in range(1, blocks - 1):
        smooth = (banded(fm[b], low_band[...]) + banded(fm[b + 1], high_band[...])) * inner
        power = power + keep(b, pl.ds(0, rows), ext[b + 1] - smooth)
    acc[...] = power

    for q, span in enumerate(spans):
        @pl.when(jnp.logical_not(is_first))
        def _():
            to_right[q].wait_recv()

        @pl.when(jnp.logical_not(is_last))
        def _():
            to_left[q].wait_recv()

        before = jnp.where(is_first, 0.0, ext[0, span])
        after = jnp.where(is_last, 0.0, ext[blocks + 1, span])
        from_before = banded(before, low_twice[...]) * (inner * inner)
        from_after = banded(after, high_twice[...]) * (inner * inner)
        power = keep(0, span, part[0, span] - from_before)
        power = power + keep(blocks - 1, span, part[1, span] - from_after)
        acc[span, :] = acc[span, :] + power

    for h in range(rows // HALF):
        turned = acc[pl.ds(h * HALF, HALF), :].T
        power_out[pl.ds(h, 1), :] = jnp.sum(turned, axis=0, keepdims=True)

    @pl.when(tm != tm_hub)
    def _():
        pl.semaphore_wait(tm_known, 1)

    late = lambda d, n: 1.5 * min(d, n - d) + (d > n // 2) + 0.5 * (d == n // 2) - 1.2 * (d == 2)
    reach = lambda p: (p[0] > 0) + 0.1 * min(p[0], other - p[0]) + late(p[1], side)
    places = sorted(((px, py) for px in range(other) for py in range(side)), key=reach)

    def to_all(src, dst, send_sem, recv_sem, order):
        for px, py in order:
            target = px * side + py
            slot = wrapped(px - tm_x + other, other) * side + wrapped(py - tm_y + side, side) - 1

            @pl.when(tm != target)
            def _():
                pltpu.make_async_remote_copy(
                    src_ref=src, dst_ref=dst.at[slot], send_sem=send_sem, recv_sem=recv_sem,
                    device_id={"tm": target}, device_id_type=MESH,
                ).start()

    to_all(power_out, power_in, power_send, power_recv, places[::-1])
    head = pltpu.make_async_remote_copy(
        src_ref=det.at[:, pl.ds(0, HALF)], dst_ref=det.at[:, pl.ds(length, HALF)],
        send_sem=head_send, recv_sem=head_recv,
        device_id={"tm": left}, device_id_type=MESH,
    )

    @pl.when(jnp.logical_not(is_first))
    def _():
        head.start()


    for b in range(blocks):
        lanes = pl.ds(b * BLOCK, BLOCK)
        for k, piece in enumerate(parts_of(det[:, lanes])):
            split[k, :, lanes] = piece
    fetch.wait()
    lane = lax.broadcasted_iota(jnp.int32, (BLOCK, HALF), 1)
    depth = lax.broadcasted_iota(jnp.int32, (BLOCK, HALF), 0)
    for i in range(boxes):
        inside = (depth >= lane) & (depth < lane + widths[i])
        for k in range(3):
            box_band[pl.ds(k * BLOCK, BLOCK), pl.ds(i * HALF, HALF)] = inside.astype(
                jnp.float32
            ).astype(jnp.bfloat16)

    def lanes_of(i, t):
        return pl.ds((i * tiles + t) * HALF, HALF)

    def box_sums(t):
        window = jnp.concatenate(
            [split[k, :, pl.ds(t * HALF, BLOCK)] for k in range(3)], axis=1
        )
        sums = jnp.dot(window, box_band[...], preferred_element_type=jnp.float32)
        for i in range(boxes):
            boxed[:, lanes_of(i, t)] = sums[:, i * HALF:(i + 1) * HALF]

    for t in range(tiles - 1):
        box_sums(t)

    @pl.when(dm != dm_hub)
    def _():
        pl.semaphore_wait(dm_known, 1)

    pltpu.make_async_copy(power_in, power_in, power_recv).wait()
    totals = power_out[...] + jnp.sum(power_in[...], axis=0)
    inverse_scale = 1.0 / jnp.sqrt(totals * (1.0 / total_len) + EPS)
    for h in range(rows // HALF):
        row = jnp.broadcast_to(inverse_scale[h:h + 1, :], (HALF, HALF))
        scale[pl.ds(h * HALF, HALF), :] = row.T

    @pl.when(jnp.logical_not(is_last))
    def _():
        head.wait_recv()

    det[:, pl.ds(length, HALF)] = jnp.where(is_last, 0.0, det[:, pl.ds(length, HALF)])
    sums = [jnp.zeros((8, HALF), jnp.float32) for _ in range(tiles + 1)]
    for r in range(rows // 8):
        gain = scale[pl.ds(r * 8, 8), :]
        for t in range(tiles + 1):
            sums[t] = sums[t] + det[pl.ds(r * 8, 8), pl.ds(t * HALF, HALF)] * gain
    for t in range(tiles + 1):
        col_out[pl.ds(t, 1), :] = jnp.sum(sums[t], axis=0, keepdims=True)
    for target in range(dm_size):

        @pl.when(dm != target)
        def _():
            pltpu.make_async_remote_copy(
                src_ref=col_out, dst_ref=col_in.at[wrapped(target - dm + dm_size, dm_size) - 1],
                send_sem=col_send, recv_sem=col_recv,
                device_id={"dm": target}, device_id_type=MESH,
            ).start()

    for k, piece in enumerate(parts_of(det[:, pl.ds(length, HALF)])):
        split[k, :, pl.ds(length, HALF)] = piece
    box_sums(tiles - 1)

    inverse = []
    for i in range(boxes):
        width = jnp.full((8, HALF), widths[i], jnp.int32).astype(jnp.float32)
        inverse.append(1.0 / jnp.sqrt(width))

    def scale_rows(r, carry):
        span = pl.ds(pl.multiple_of(r * 8, 8), 8)
        gain = scale[span, :]
        for i in range(boxes):
            gain_i = gain * inverse[i]
            for t in range(tiles):
                boxed[span, lanes_of(i, t)] = boxed[span, lanes_of(i, t)] * gain_i
        return carry

    lax.fori_loop(0, rows // 8, scale_rows, 0)

    pltpu.make_async_copy(col_in, col_in, col_recv).wait()
    column_total = col_out[...] + jnp.sum(col_in[...], axis=0)
    common[...] = column_total * (1.0 / (rows * dm_size))
    window = jnp.concatenate([common[pl.ds(0, tiles), :], common[pl.ds(1, tiles), :]], axis=1)
    box_common[...] = banded(window, box_band[pl.ds(0, BLOCK), :])

    halves = rows // HALF
    offsets = [
        [
            jnp.broadcast_to(box_common[pl.ds(t, 1), pl.ds(i * HALF, HALF)], (8, HALF)) * inverse[i]
            for t in range(tiles)
        ]
        for i in range(boxes)
    ]

    def series_of(i, t, span):
        return boxed[span, lanes_of(i, t)] - offsets[i][t]

    for i in range(boxes):
        for h in range(halves):
            pieces = []
            for r in range(HALF // 8):
                span = pl.ds(h * HALF + r * 8, 8)
                values = [series_of(i, t, span) for t in range(tiles)]
                while len(values) > 1:
                    values = [jnp.maximum(a, b) for a, b in zip(values[::2], values[1::2])]
                pieces.append(values[0])
            turned = jnp.concatenate(pieces, axis=0).T
            peak_out[pl.ds(i * halves + h, 1), :] = jnp.max(turned, axis=0, keepdims=True)
    to_all(peak_out, peak_in, peak_send, peak_recv, places)

    for i in range(boxes):

        def some_rows(r, carry):
            top = pl.ds(pl.multiple_of(r * 16, 16), 8)
            bottom = pl.ds(pl.multiple_of(r * 16 + 8, 8), 8)
            both = pl.ds(pl.multiple_of(r * 16, 16), 16)
            for t in range(tiles):
                pair = jnp.concatenate([series_of(i, t, top), series_of(i, t, bottom)], axis=0)
                snr[i, both, pl.ds(t * HALF, HALF)] = pair.astype(jnp.bfloat16)
            return carry

        lax.fori_loop(0, rows // 16, some_rows, 0)

    pltpu.make_async_copy(peak_in, peak_in, peak_recv).wait()
    most = jnp.maximum(peak_out[...], jnp.max(peak_in[...], axis=0))
    for i in range(boxes):
        for h in range(halves):
            row = i * halves + h
            peaks[pl.ds(i, 1), pl.ds(h * HALF, HALF)] = most[row:row + 1, :]

    @pl.when(jnp.logical_not(is_last))
    def _():
        for copy in to_right:
            copy.wait_send()

    @pl.when(jnp.logical_not(is_first))
    def _():
        for copy in to_left:
            copy.wait_send()
        head.wait_send()

    pltpu.make_async_copy(power_in, power_in, power_send).wait()
    pltpu.make_async_copy(col_in, col_in, col_send).wait()
    pltpu.make_async_copy(peak_in, peak_in, peak_send).wait()


def hand_out(snr, peaks, snr_out, peaks_out, peaks_sem, sems):
    boxes, pieces = sems.shape
    rows = snr.shape[1] // pieces
    copies = [pltpu.make_async_copy(peaks, peaks_out, peaks_sem)]
    for i in range(boxes):
        for k in range(pieces):
            span = pl.ds(k * rows, rows)
            copies.append(pltpu.make_async_copy(snr.at[i, span], snr_out.at[i, span], sems.at[i, k]))
    for copy in copies:
        copy.start()
    for copy in copies:
        copy.wait()


def solution(mesh):
    tm_size, dm_size = mesh.shape["tm"], mesh.shape["dm"]

    def step(dispersed, widths):
        rows, length = dispersed.shape
        boxes = widths.shape[0]
        blocks, tiles, halves = length // BLOCK, length // HALF, rows // HALF
        f32, bf16 = jnp.float32, jnp.bfloat16
        dma = pltpu.SemaphoreType.DMA
        inputs = [pltpu.with_memory_space_constraint(a, pltpu.HBM) for a in (widths, dispersed)]
        snr, peaks = pl.pallas_call(
            functools.partial(kernel, tm_size, dm_size),
            out_shape=(
                pltpu.VMEM((boxes, rows, length), bf16),
                pltpu.VMEM((boxes, rows), f32),
            ),
            in_specs=[pl.BlockSpec(memory_space=pltpu.HBM)] * 2,
            out_specs=(pl.BlockSpec(memory_space=pltpu.VMEM),) * 2,
            scratch_shapes=[
                pltpu.SMEM((boxes,), jnp.int32),
                dma,
                pltpu.VMEM((blocks + 2, rows, BLOCK), f32),
                pltpu.VMEM((BLOCK, BLOCK), bf16),
                pltpu.VMEM((BLOCK, BLOCK), bf16),
                pltpu.VMEM((BLOCK, BLOCK), bf16),
                pltpu.VMEM((BLOCK, BLOCK), bf16),
                pltpu.VMEM((3 * BLOCK, boxes * HALF), bf16),
                pltpu.VMEM((blocks, rows, BLOCK), f32),
                pltpu.VMEM((2, rows, BLOCK), f32),
                pltpu.VMEM((rows, length + HALF), f32),
                pltpu.VMEM((3, rows, length + HALF), bf16),
                pltpu.VMEM((rows, boxes * tiles * HALF), f32),
                pltpu.VMEM((rows, HALF), f32),
                pltpu.VMEM((halves, HALF), f32),
                pltpu.VMEM((tm_size - 1, halves, HALF), f32),
                pltpu.VMEM((rows, HALF), f32),
                pltpu.VMEM((tiles + 1, HALF), f32),
                pltpu.VMEM((dm_size - 1, tiles + 1, HALF), f32),
                pltpu.VMEM((tiles + 1, HALF), f32),
                pltpu.VMEM((tiles, boxes * HALF), f32),
                pltpu.VMEM((boxes * halves, HALF), f32),
                pltpu.VMEM((tm_size - 1, boxes * halves, HALF), f32),
                dma((2, len(CHUNKS))),
                dma((blocks,)),
                dma((2, len(CHUNKS))),
                dma((2, len(CHUNKS))),
                dma, dma, dma, dma, dma, dma, dma, dma,
                pltpu.SemaphoreType.REGULAR,
                pltpu.SemaphoreType.REGULAR,
            ],
            compiler_params=pltpu.CompilerParams(
                collective_id=0, has_side_effects=True, vmem_limit_bytes=48 * 2**20
            ),
        )(*inputs)
        return pl.pallas_call(
            hand_out,
            out_shape=(
                jax.ShapeDtypeStruct(snr.shape, bf16),
                jax.ShapeDtypeStruct(peaks.shape, f32),
            ),
            in_specs=[pl.BlockSpec(memory_space=pl.ANY)] * 2,
            out_specs=(pl.BlockSpec(memory_space=pl.ANY),) * 2,
            scratch_shapes=[dma, dma((boxes, 1))],
            compiler_params=pltpu.CompilerParams(vmem_limit_bytes=2**22),
        )(snr, peaks)

    return jax.shard_map(
        step,
        mesh=mesh,
        in_specs=(P("dm", "tm"), P()),
        out_specs=(P(None, "dm", "tm"), P(None, "dm")),
        check_vma=False,
    )
```

```python
import functools

import jax
import jax.numpy as jnp
from jax import lax
from jax.experimental import pallas as pl
from jax.experimental.pallas import tpu as pltpu
from jax.sharding import PartitionSpec as P

MESH = pl.DeviceIdType.MESH
HALF = 128
BLOCK = 2 * HALF
EPS = 1e-06
CHUNKS = (96, 96, 48, 16)


def parts_of(x):
    high = x.astype(jnp.bfloat16)
    rest = x - high.astype(jnp.float32)
    mid = rest.astype(jnp.bfloat16)
    low = (rest - mid.astype(jnp.float32)).astype(jnp.bfloat16)
    return high, mid, low


def banded(x, band):
    rows = x.shape[0]
    stacked = jnp.concatenate(parts_of(x), axis=0)
    sums = jnp.dot(stacked, band, preferred_element_type=jnp.float32)
    return sums[:rows] + sums[rows:2 * rows] + sums[2 * rows:]


def wrapped(index, size):
    return jnp.where(index >= size, index - size, index)


def peer_offsets(peers):
    side = 8 if peers % 8 == 0 else peers
    other = peers // side
    steps = [(dx, dy) for dx in range(other) for dy in range(side) if dx or dy]
    reach = lambda s: min(s[0], other - s[0]) + min(s[1], side - s[1])
    return side, other, sorted(steps, key=reach, reverse=True)


def kernel(
    tm_size, dm_size, widths_in, x, snr, peaks,
    widths, widths_sem, ext, low_band, high_band, low_twice, high_twice, box_band, fm, part, det, split, boxed, acc,
    power_out, power_in, scale, col_out, col_in, common, box_common, peak_out, peak_in,
    edge_sem, load_sem, halo_send, halo_recv, head_send, head_recv,
    power_send, power_recv, col_send, col_recv, peak_send, peak_recv, tm_known, dm_known,
):
    rows, length = x.shape
    boxes = widths.shape[0]
    blocks = length // BLOCK
    tiles = length // HALF
    total_len = length * tm_size
    tm = lax.axis_index("tm")
    dm = lax.axis_index("dm")
    right, left = wrapped(tm + 1, tm_size), wrapped(tm + tm_size - 1, tm_size)
    side, other, steps = peer_offsets(tm_size)
    tm_x = tm // side
    tm_y = tm - tm_x * side

    def tm_peer(step):
        return wrapped(tm_x + step[0], other) * side + wrapped(tm_y + step[1], side)


    dm_hub = dm_size - 1
    hub_x, hub_y = other // 2, (side // 2 + 1) % side
    tm_hub = hub_x * side + hub_y
    is_first, is_last = tm == 0, tm == tm_size - 1
    near_hub = (tm >= tm_hub - 1) & (tm <= tm_hub + 1)
    barrier = pltpu.get_barrier_semaphore()

    def greet(peer):
        pl.semaphore_signal(barrier, inc=1, device_id=peer, device_id_type=MESH)

    @pl.when(jnp.logical_not(is_first))
    def _():
        greet({"tm": left})

    @pl.when(jnp.logical_not(is_last))
    def _():
        greet({"tm": right})

    @pl.when(jnp.logical_not(near_hub))
    def _():
        greet({"tm": tm_hub})

    @pl.when(dm != dm_hub)
    def _():
        greet({"dm": dm_hub})

    spans = [pl.ds(sum(CHUNKS[:q]), CHUNKS[q]) for q in range(len(CHUNKS))]
    edge_loads = []
    for q, span in enumerate(spans):
        for b in (blocks, 1):
            edge_loads.append(
                pltpu.make_async_copy(
                    x.at[span, pl.ds((b - 1) * BLOCK, BLOCK)], ext.at[b, span],
                    edge_sem.at[int(b == 1), q],
                )
            )
            edge_loads[-1].start()

    beside = jnp.minimum(tm, 1) + jnp.minimum(tm_size - 1 - tm, 1)
    greetings = jnp.where(tm == tm_hub, tm_size - 1, beside)
    greetings = greetings + jnp.where(dm == dm_hub, dm_size - 1, 0)

    for load in edge_loads[:2]:
        load.wait()
    pl.semaphore_wait(barrier, greetings)
    to_right, to_left = [], []
    for q, span in enumerate(spans):
        to_right.append(
            pltpu.make_async_remote_copy(
                src_ref=ext.at[blocks, span], dst_ref=ext.at[0, span],
                send_sem=halo_send.at[0, q], recv_sem=halo_recv.at[0, q],
                device_id={"tm": right}, device_id_type=MESH,
            )
        )
        to_left.append(
            pltpu.make_async_remote_copy(
                src_ref=ext.at[1, span], dst_ref=ext.at[blocks + 1, span],
                send_sem=halo_send.at[1, q], recv_sem=halo_recv.at[1, q],
                device_id={"tm": left}, device_id_type=MESH,
            )
        )
    for q in range(len(spans)):
        if q > 0:
            edge_loads[2 * q].wait()
            edge_loads[2 * q + 1].wait()

        @pl.when(jnp.logical_not(is_last))
        def _():
            to_right[q].start()

        @pl.when(jnp.logical_not(is_first))
        def _():
            to_left[q].start()

    loads = {}
    for b in range(2, blocks):
        loads[b] = pltpu.make_async_copy(
            x.at[:, pl.ds((b - 1) * BLOCK, BLOCK)], ext.at[b], load_sem.at[b - 1]
        )
        loads[b].start()
    fetch = pltpu.make_async_copy(widths_in, widths, widths_sem)
    fetch.start()

    @pl.when(tm == tm_hub)
    def _():
        for step in steps:
            pl.semaphore_signal(
                tm_known, inc=1, device_id={"tm": tm_peer(step)}, device_id_type=MESH
            )

    @pl.when(dm == dm_hub)
    def _():
        for d in range(dm_size - 1):
            pl.semaphore_signal(dm_known, inc=1, device_id={"dm": d}, device_id_type=MESH)

    row_idx = lax.broadcasted_iota(jnp.int32, (BLOCK, BLOCK), 0)
    col_idx = lax.broadcasted_iota(jnp.int32, (BLOCK, BLOCK), 1)
    low = (row_idx >= col_idx).astype(jnp.float32).astype(jnp.bfloat16)
    high = (row_idx <= col_idx).astype(jnp.float32).astype(jnp.bfloat16)
    low_band[...] = low
    high_band[...] = high
    span_len = (row_idx - col_idx).astype(jnp.float32)
    low_twice[...] = jnp.maximum(span_len + 1.0, 0.0).astype(jnp.bfloat16)
    high_twice[...] = jnp.maximum(1.0 - span_len, 0.0).astype(jnp.bfloat16)

    def inverse_counts(first):
        pos = first + lax.broadcasted_iota(jnp.int32, (1, BLOCK), 1)
        counts = (jnp.minimum(pos + HALF, total_len - 1) - jnp.maximum(pos - HALF, 0) + 1)
        valid = (pos >= 0) & (pos < total_len)
        return jnp.where(valid, 1.0 / jnp.maximum(counts, 1).astype(jnp.float32), 0.0)

    offset = tm * length
    inner = 1.0 / (2 * HALF + 1)
    edge_first = inverse_counts(offset - HALF)
    edge_last = inverse_counts(offset + length - HALF)
    own_first = inverse_counts(offset)
    own_last = inverse_counts(offset + length - BLOCK)

    for b in range(2, blocks):
        loads[b].wait()
    for b in range(1, blocks):
        sums = banded(ext[b], low_band[...]) + banded(ext[b + 1], high_band[...])
        fm[b] = sums * inner
    mean = banded(ext[1], high_band[...]) * edge_first
    smooth = banded(fm[1], high_band[...]) + banded(mean, low_band[...])
    part[0] = ext[1] - smooth * own_first
    mean = banded(ext[blocks], low_band[...]) * edge_last
    smooth = banded(fm[blocks - 1], low_band[...]) + banded(mean, high_band[...])
    part[1] = ext[blocks] - smooth * own_last

    def keep(block_idx, span, values):
        det[span, pl.ds(block_idx * BLOCK, BLOCK)] = values
        squares = values * values
        return squares[:, :HALF] + squares[:, HALF:]

    power = jnp.zeros((rows, HALF), jnp.float32)
    for b in range(1, blocks - 1):
        smooth = (banded(fm[b], low_band[...]) + banded(fm[b + 1], high_band[...])) * inner
        power = power + keep(b, pl.ds(0, rows), ext[b + 1] - smooth)
    acc[...] = power

    for q, span in enumerate(spans):
        @pl.when(jnp.logical_not(is_first))
        def _():
            to_right[q].wait_recv()

        @pl.when(jnp.logical_not(is_last))
        def _():
            to_left[q].wait_recv()

        before = jnp.where(is_first, 0.0, ext[0, span] * (inner * inner))
        after = jnp.where(is_last, 0.0, ext[blocks + 1, span] * (inner * inner))
        from_before = banded(before, low_twice[...])
        from_after = banded(after, high_twice[...])
        power = keep(0, span, part[0, span] - from_before)
        power = power + keep(blocks - 1, span, part[1, span] - from_after)
        acc[span, :] = acc[span, :] + power

    for h in range(rows // HALF):
        turned = acc[pl.ds(h * HALF, HALF), :].T
        power_out[pl.ds(h, 1), :] = jnp.sum(turned, axis=0, keepdims=True)

    @pl.when(tm != tm_hub)
    def _():
        pl.semaphore_wait(tm_known, 1)

    late = lambda d, n: 1.5 * min(d, n - d) + (d > n // 2) + 0.5 * (d == n // 2) - 1.2 * (d == 2)
    reach = lambda p: (p[0] > 0) + 0.1 * min(p[0], other - p[0]) + late(p[1], side)
    places = sorted(((px, py) for px in range(other) for py in range(side)), key=reach)

    def to_all(src, dst, send_sem, recv_sem, order):
        for px, py in order:
            target = px * side + py
            slot = wrapped(px - tm_x + other, other) * side + wrapped(py - tm_y + side, side) - 1

            @pl.when(tm != target)
            def _():
                pltpu.make_async_remote_copy(
                    src_ref=src, dst_ref=dst.at[slot], send_sem=send_sem, recv_sem=recv_sem,
                    device_id={"tm": target}, device_id_type=MESH,
                ).start()

    to_all(power_out, power_in, power_send, power_recv, places[::-1])
    head = pltpu.make_async_remote_copy(
        src_ref=det.at[:, pl.ds(0, HALF)], dst_ref=det.at[:, pl.ds(length, HALF)],
        send_sem=head_send, recv_sem=head_recv,
        device_id={"tm": left}, device_id_type=MESH,
    )

    @pl.when(jnp.logical_not(is_first))
    def _():
        head.start()


    for b in range(blocks):
        lanes = pl.ds(b * BLOCK, BLOCK)
        for k, piece in enumerate(parts_of(det[:, lanes])):
            split[k, :, lanes] = piece
    fetch.wait()
    lane = lax.broadcasted_iota(jnp.int32, (BLOCK, HALF), 1)
    depth = lax.broadcasted_iota(jnp.int32, (BLOCK, HALF), 0)
    for i in range(boxes):
        inside = (depth >= lane) & (depth < lane + widths[i])
        for k in range(3):
            box_band[pl.ds(k * BLOCK, BLOCK), pl.ds(i * HALF, HALF)] = inside.astype(
                jnp.float32
            ).astype(jnp.bfloat16)

    def lanes_of(i, t):
        return pl.ds((i * tiles + t) * HALF, HALF)

    def box_sums(t):
        window = jnp.concatenate(
            [split[k, :, pl.ds(t * HALF, BLOCK)] for k in range(3)], axis=1
        )
        sums = jnp.dot(window, box_band[...], preferred_element_type=jnp.float32)
        for i in range(boxes):
            boxed[:, lanes_of(i, t)] = sums[:, i * HALF:(i + 1) * HALF]

    for t in range(tiles - 1):
        box_sums(t)

    @pl.when(dm != dm_hub)
    def _():
        pl.semaphore_wait(dm_known, 1)

    pltpu.make_async_copy(power_in, power_in, power_recv).wait()
    totals = power_out[...] + jnp.sum(power_in[...], axis=0)
    inverse_scale = 1.0 / jnp.sqrt(totals * (1.0 / total_len) + EPS)
    for h in range(rows // HALF):
        row = jnp.broadcast_to(inverse_scale[h:h + 1, :], (HALF, HALF))
        scale[pl.ds(h * HALF, HALF), :] = row.T

    @pl.when(jnp.logical_not(is_last))
    def _():
        head.wait_recv()

    det[:, pl.ds(length, HALF)] = jnp.where(is_last, 0.0, det[:, pl.ds(length, HALF)])
    sums = [jnp.zeros((8, HALF), jnp.float32) for _ in range(tiles + 1)]
    for r in range(rows // 8):
        gain = scale[pl.ds(r * 8, 8), :]
        for t in range(tiles + 1):
            sums[t] = sums[t] + det[pl.ds(r * 8, 8), pl.ds(t * HALF, HALF)] * gain
    for t in range(tiles + 1):
        col_out[pl.ds(t, 1), :] = jnp.sum(sums[t], axis=0, keepdims=True)
    for target in range(dm_size):

        @pl.when(dm != target)
        def _():
            pltpu.make_async_remote_copy(
                src_ref=col_out, dst_ref=col_in.at[wrapped(target - dm + dm_size, dm_size) - 1],
                send_sem=col_send, recv_sem=col_recv,
                device_id={"dm": target}, device_id_type=MESH,
            ).start()

    for k, piece in enumerate(parts_of(det[:, pl.ds(length, HALF)])):
        split[k, :, pl.ds(length, HALF)] = piece
    box_sums(tiles - 1)

    inverse = []
    for i in range(boxes):
        width = jnp.full((8, HALF), widths[i], jnp.int32).astype(jnp.float32)
        inverse.append(1.0 / jnp.sqrt(width))

    def scale_rows(r, carry):
        span = pl.ds(pl.multiple_of(r * 8, 8), 8)
        gain = scale[span, :]
        for i in range(boxes):
            gain_i = gain * inverse[i]
            for t in range(tiles):
                boxed[span, lanes_of(i, t)] = boxed[span, lanes_of(i, t)] * gain_i
        return carry

    lax.fori_loop(0, rows // 8, scale_rows, 0)

    pltpu.make_async_copy(col_in, col_in, col_recv).wait()
    column_total = col_out[...] + jnp.sum(col_in[...], axis=0)
    common[...] = column_total * (1.0 / (rows * dm_size))
    window = jnp.concatenate([common[pl.ds(0, tiles), :], common[pl.ds(1, tiles), :]], axis=1)
    box_common[...] = banded(window, box_band[pl.ds(0, BLOCK), :])

    halves = rows // HALF
    offsets = [
        [
            jnp.broadcast_to(box_common[pl.ds(t, 1), pl.ds(i * HALF, HALF)], (8, HALF)) * inverse[i]
            for t in range(tiles)
        ]
        for i in range(boxes)
    ]

    def series_of(i, t, span):
        return boxed[span, lanes_of(i, t)] - offsets[i][t]

    for i in range(boxes):
        for h in range(halves):
            pieces = []
            for r in range(HALF // 8):
                span = pl.ds(h * HALF + r * 8, 8)
                values = [series_of(i, t, span) for t in range(tiles)]
                while len(values) > 1:
                    values = [jnp.maximum(a, b) for a, b in zip(values[::2], values[1::2])]
                pieces.append(values[0])
            turned = jnp.concatenate(pieces, axis=0).T
            peak_out[pl.ds(i * halves + h, 1), :] = jnp.max(turned, axis=0, keepdims=True)
    to_all(peak_out, peak_in, peak_send, peak_recv, places)

    for i in range(boxes):

        def some_rows(r, carry):
            top = pl.ds(pl.multiple_of(r * 16, 16), 8)
            bottom = pl.ds(pl.multiple_of(r * 16 + 8, 8), 8)
            both = pl.ds(pl.multiple_of(r * 16, 16), 16)
            for t in range(tiles):
                pair = jnp.concatenate([series_of(i, t, top), series_of(i, t, bottom)], axis=0)
                snr[i, both, pl.ds(t * HALF, HALF)] = pair.astype(jnp.bfloat16)
            return carry

        lax.fori_loop(0, rows // 16, some_rows, 0)

    pltpu.make_async_copy(peak_in, peak_in, peak_recv).wait()
    most = jnp.maximum(peak_out[...], jnp.max(peak_in[...], axis=0))
    for i in range(boxes):
        for h in range(halves):
            row = i * halves + h
            peaks[pl.ds(i, 1), pl.ds(h * HALF, HALF)] = most[row:row + 1, :]

    @pl.when(jnp.logical_not(is_last))
    def _():
        for copy in to_right:
            copy.wait_send()

    @pl.when(jnp.logical_not(is_first))
    def _():
        for copy in to_left:
            copy.wait_send()
        head.wait_send()

    pltpu.make_async_copy(power_in, power_in, power_send).wait()
    pltpu.make_async_copy(col_in, col_in, col_send).wait()
    pltpu.make_async_copy(peak_in, peak_in, peak_send).wait()


def hand_out(snr, peaks, snr_out, peaks_out, peaks_sem, sems):
    boxes, pieces = sems.shape
    rows = snr.shape[1] // pieces
    copies = [pltpu.make_async_copy(peaks, peaks_out, peaks_sem)]
    for i in range(boxes):
        for k in range(pieces):
            span = pl.ds(k * rows, rows)
            copies.append(pltpu.make_async_copy(snr.at[i, span], snr_out.at[i, span], sems.at[i, k]))
    for copy in copies:
        copy.start()
    for copy in copies:
        copy.wait()


def solution(mesh):
    tm_size, dm_size = mesh.shape["tm"], mesh.shape["dm"]

    def step(dispersed, widths):
        rows, length = dispersed.shape
        boxes = widths.shape[0]
        blocks, tiles, halves = length // BLOCK, length // HALF, rows // HALF
        f32, bf16 = jnp.float32, jnp.bfloat16
        dma = pltpu.SemaphoreType.DMA
        inputs = [pltpu.with_memory_space_constraint(a, pltpu.HBM) for a in (widths, dispersed)]
        snr, peaks = pl.pallas_call(
            functools.partial(kernel, tm_size, dm_size),
            out_shape=(
                pltpu.VMEM((boxes, rows, length), bf16),
                pltpu.VMEM((boxes, rows), f32),
            ),
            in_specs=[pl.BlockSpec(memory_space=pltpu.HBM)] * 2,
            out_specs=(pl.BlockSpec(memory_space=pltpu.VMEM),) * 2,
            scratch_shapes=[
                pltpu.SMEM((boxes,), jnp.int32),
                dma,
                pltpu.VMEM((blocks + 2, rows, BLOCK), f32),
                pltpu.VMEM((BLOCK, BLOCK), bf16),
                pltpu.VMEM((BLOCK, BLOCK), bf16),
                pltpu.VMEM((BLOCK, BLOCK), bf16),
                pltpu.VMEM((BLOCK, BLOCK), bf16),
                pltpu.VMEM((3 * BLOCK, boxes * HALF), bf16),
                pltpu.VMEM((blocks, rows, BLOCK), f32),
                pltpu.VMEM((2, rows, BLOCK), f32),
                pltpu.VMEM((rows, length + HALF), f32),
                pltpu.VMEM((3, rows, length + HALF), bf16),
                pltpu.VMEM((rows, boxes * tiles * HALF), f32),
                pltpu.VMEM((rows, HALF), f32),
                pltpu.VMEM((halves, HALF), f32),
                pltpu.VMEM((tm_size - 1, halves, HALF), f32),
                pltpu.VMEM((rows, HALF), f32),
                pltpu.VMEM((tiles + 1, HALF), f32),
                pltpu.VMEM((dm_size - 1, tiles + 1, HALF), f32),
                pltpu.VMEM((tiles + 1, HALF), f32),
                pltpu.VMEM((tiles, boxes * HALF), f32),
                pltpu.VMEM((boxes * halves, HALF), f32),
                pltpu.VMEM((tm_size - 1, boxes * halves, HALF), f32),
                dma((2, len(CHUNKS))),
                dma((blocks,)),
                dma((2, len(CHUNKS))),
                dma((2, len(CHUNKS))),
                dma, dma, dma, dma, dma, dma, dma, dma,
                pltpu.SemaphoreType.REGULAR,
                pltpu.SemaphoreType.REGULAR,
            ],
            compiler_params=pltpu.CompilerParams(
                collective_id=0, has_side_effects=True, vmem_limit_bytes=48 * 2**20
            ),
        )(*inputs)
        return pl.pallas_call(
            hand_out,
            out_shape=(
                jax.ShapeDtypeStruct(snr.shape, bf16),
                jax.ShapeDtypeStruct(peaks.shape, f32),
            ),
            in_specs=[pl.BlockSpec(memory_space=pl.ANY)] * 2,
            out_specs=(pl.BlockSpec(memory_space=pl.ANY),) * 2,
            scratch_shapes=[dma, dma((boxes, 1))],
            compiler_params=pltpu.CompilerParams(vmem_limit_bytes=2**22),
        )(snr, peaks)

    return jax.shard_map(
        step,
        mesh=mesh,
        in_specs=(P("dm", "tm"), P()),
        out_specs=(P(None, "dm", "tm"), P(None, "dm")),
        check_vma=False,
    )
```

```python
import functools

import jax
import jax.numpy as jnp
from jax import lax
from jax.experimental import pallas as pl
from jax.experimental.pallas import tpu as pltpu
from jax.sharding import PartitionSpec as P

MESH = pl.DeviceIdType.MESH
HALF = 128
BLOCK = 2 * HALF
EPS = 1e-06
CHUNKS = (96, 96, 48, 16)


def parts_of(x):
    high = x.astype(jnp.bfloat16)
    rest = x - high.astype(jnp.float32)
    mid = rest.astype(jnp.bfloat16)
    low = (rest - mid.astype(jnp.float32)).astype(jnp.bfloat16)
    return high, mid, low


def banded(x, band):
    rows = x.shape[0]
    stacked = jnp.concatenate(parts_of(x), axis=0)
    sums = jnp.dot(stacked, band, preferred_element_type=jnp.float32)
    return sums[:rows] + sums[rows:2 * rows] + sums[2 * rows:]


def wrapped(index, size):
    return jnp.where(index >= size, index - size, index)


def peer_offsets(peers):
    side = 8 if peers % 8 == 0 else peers
    other = peers // side
    steps = [(dx, dy) for dx in range(other) for dy in range(side) if dx or dy]
    reach = lambda s: min(s[0], other - s[0]) + min(s[1], side - s[1])
    return side, other, sorted(steps, key=reach, reverse=True)


def kernel(
    tm_size, dm_size, widths_in, x, snr, peaks,
    widths, widths_sem, ext, low_band, high_band, low_twice, high_twice, box_band, fm, part, det, split, boxed, acc,
    power_out, power_in, scale, col_out, col_in, common, box_common, peak_out, peak_in,
    edge_sem, load_sem, halo_send, halo_recv, head_send, head_recv,
    power_send, power_recv, col_send, col_recv, peak_send, peak_recv, tm_known, dm_known,
):
    rows, length = x.shape
    boxes = widths.shape[0]
    blocks = length // BLOCK
    tiles = length // HALF
    total_len = length * tm_size
    tm = lax.axis_index("tm")
    dm = lax.axis_index("dm")
    right, left = wrapped(tm + 1, tm_size), wrapped(tm + tm_size - 1, tm_size)
    side, other, steps = peer_offsets(tm_size)
    tm_x = tm // side
    tm_y = tm - tm_x * side

    def tm_peer(step):
        return wrapped(tm_x + step[0], other) * side + wrapped(tm_y + step[1], side)


    dm_hub = dm_size - 1
    hub_x, hub_y = other // 2, (side // 2 + 1) % side
    tm_hub = hub_x * side + hub_y
    is_first, is_last = tm == 0, tm == tm_size - 1
    near_hub = (tm >= tm_hub - 1) & (tm <= tm_hub + 1)
    barrier = pltpu.get_barrier_semaphore()

    def greet(peer):
        pl.semaphore_signal(barrier, inc=1, device_id=peer, device_id_type=MESH)

    @pl.when(jnp.logical_not(is_first))
    def _():
        greet({"tm": left})

    @pl.when(jnp.logical_not(is_last))
    def _():
        greet({"tm": right})

    @pl.when(jnp.logical_not(near_hub))
    def _():
        greet({"tm": tm_hub})

    @pl.when(dm != dm_hub)
    def _():
        greet({"dm": dm_hub})

    spans = [pl.ds(sum(CHUNKS[:q]), CHUNKS[q]) for q in range(len(CHUNKS))]
    edge_loads = []
    for q, span in enumerate(spans):
        for b in (blocks, 1):
            edge_loads.append(
                pltpu.make_async_copy(
                    x.at[span, pl.ds((b - 1) * BLOCK, BLOCK)], ext.at[b, span],
                    edge_sem.at[int(b == 1), q],
                )
            )
            edge_loads[-1].start()

    beside = jnp.minimum(tm, 1) + jnp.minimum(tm_size - 1 - tm, 1)
    greetings = jnp.where(tm == tm_hub, tm_size - 1, beside)
    greetings = greetings + jnp.where(dm == dm_hub, dm_size - 1, 0)

    for load in edge_loads[:2]:
        load.wait()
    pl.semaphore_wait(barrier, greetings)
    to_right, to_left = [], []
    for q, span in enumerate(spans):
        to_right.append(
            pltpu.make_async_remote_copy(
                src_ref=ext.at[blocks, span], dst_ref=ext.at[0, span],
                send_sem=halo_send.at[0, q], recv_sem=halo_recv.at[0, q],
                device_id={"tm": right}, device_id_type=MESH,
            )
        )
        to_left.append(
            pltpu.make_async_remote_copy(
                src_ref=ext.at[1, span], dst_ref=ext.at[blocks + 1, span],
                send_sem=halo_send.at[1, q], recv_sem=halo_recv.at[1, q],
                device_id={"tm": left}, device_id_type=MESH,
            )
        )
    for q in range(len(spans)):
        if q > 0:
            edge_loads[2 * q].wait()
            edge_loads[2 * q + 1].wait()

        @pl.when(jnp.logical_not(is_last))
        def _():
            to_right[q].start()

        @pl.when(jnp.logical_not(is_first))
        def _():
            to_left[q].start()

    loads = {}
    for b in range(2, blocks):
        loads[b] = pltpu.make_async_copy(
            x.at[:, pl.ds((b - 1) * BLOCK, BLOCK)], ext.at[b], load_sem.at[b - 1]
        )
        loads[b].start()
    fetch = pltpu.make_async_copy(widths_in, widths, widths_sem)
    fetch.start()

    @pl.when(tm == tm_hub)
    def _():
        for step in steps:
            pl.semaphore_signal(
                tm_known, inc=1, device_id={"tm": tm_peer(step)}, device_id_type=MESH
            )

    @pl.when(dm == dm_hub)
    def _():
        for d in range(dm_size - 1):
            pl.semaphore_signal(dm_known, inc=1, device_id={"dm": d}, device_id_type=MESH)

    row_idx = lax.broadcasted_iota(jnp.int32, (BLOCK, BLOCK), 0)
    col_idx = lax.broadcasted_iota(jnp.int32, (BLOCK, BLOCK), 1)
    low = (row_idx >= col_idx).astype(jnp.float32).astype(jnp.bfloat16)
    high = (row_idx <= col_idx).astype(jnp.float32).astype(jnp.bfloat16)
    low_band[...] = low
    high_band[...] = high
    span_len = (row_idx - col_idx).astype(jnp.float32)
    low_twice[...] = jnp.maximum(span_len + 1.0, 0.0).astype(jnp.bfloat16)
    high_twice[...] = jnp.maximum(1.0 - span_len, 0.0).astype(jnp.bfloat16)

    def inverse_counts(first):
        pos = first + lax.broadcasted_iota(jnp.int32, (1, BLOCK), 1)
        counts = (jnp.minimum(pos + HALF, total_len - 1) - jnp.maximum(pos - HALF, 0) + 1)
        valid = (pos >= 0) & (pos < total_len)
        return jnp.where(valid, 1.0 / jnp.maximum(counts, 1).astype(jnp.float32), 0.0)

    offset = tm * length
    inner = 1.0 / (2 * HALF + 1)
    edge_first = inverse_counts(offset - HALF)
    edge_last = inverse_counts(offset + length - HALF)
    own_first = inverse_counts(offset)
    own_last = inverse_counts(offset + length - BLOCK)

    for b in range(2, blocks):
        loads[b].wait()
    for b in range(1, blocks):
        sums = banded(ext[b], low_band[...]) + banded(ext[b + 1], high_band[...])
        fm[b] = sums * inner
    mean = banded(ext[1], high_band[...]) * edge_first
    smooth = banded(fm[1], high_band[...]) + banded(mean, low_band[...])
    part[0] = ext[1] - smooth * own_first
    mean = banded(ext[blocks], low_band[...]) * edge_last
    smooth = banded(fm[blocks - 1], low_band[...]) + banded(mean, high_band[...])
    part[1] = ext[blocks] - smooth * own_last

    def keep(block_idx, span, values):
        det[span, pl.ds(block_idx * BLOCK, BLOCK)] = values
        squares = values * values
        return squares[:, :HALF] + squares[:, HALF:]

    power = jnp.zeros((rows, HALF), jnp.float32)
    for b in range(1, blocks - 1):
        smooth = (banded(fm[b], low_band[...]) + banded(fm[b + 1], high_band[...])) * inner
        power = power + keep(b, pl.ds(0, rows), ext[b + 1] - smooth)
    acc[...] = power

    for q, span in enumerate(spans):
        @pl.when(jnp.logical_not(is_first))
        def _():
            to_right[q].wait_recv()

        @pl.when(jnp.logical_not(is_last))
        def _():
            to_left[q].wait_recv()

        before = jnp.where(is_first, 0.0, ext[0, span] * (inner * inner))
        after = jnp.where(is_last, 0.0, ext[blocks + 1, span] * (inner * inner))
        from_before = banded(before, low_twice[...])
        from_after = banded(after, high_twice[...])
        power = keep(0, span, part[0, span] - from_before)
        power = power + keep(blocks - 1, span, part[1, span] - from_after)
        acc[span, :] = acc[span, :] + power

    for h in range(rows // HALF):
        turned = acc[pl.ds(h * HALF, HALF), :].T
        power_out[pl.ds(h, 1), :] = jnp.sum(turned, axis=0, keepdims=True)

    @pl.when(tm != tm_hub)
    def _():
        pl.semaphore_wait(tm_known, 1)

    late = lambda d, n: 1.5 * min(d, n - d) + (d > n // 2) + 0.5 * (d == n // 2) - 1.2 * (d == 2)
    reach = lambda p: (p[0] > 0) + 0.1 * min(p[0], other - p[0]) + late(p[1], side)
    places = sorted(((px, py) for px in range(other) for py in range(side)), key=reach)

    def to_all(src, dst, send_sem, recv_sem, order):
        names = [px * side + py for px, py in order]
        rank = sum(jnp.where(tm == name, k, 0) for k, name in enumerate(names))
        for k in range(tm_size - 1):
            target = jnp.where(rank <= k, names[k + 1], names[k])
            pltpu.make_async_remote_copy(
                src_ref=src, dst_ref=dst.at[tm - jnp.where(tm > target, 1, 0)],
                send_sem=send_sem, recv_sem=recv_sem,
                device_id={"tm": target}, device_id_type=MESH,
            ).start()

    to_all(power_out, power_in, power_send, power_recv, places[::-1])
    head = pltpu.make_async_remote_copy(
        src_ref=det.at[:, pl.ds(0, HALF)], dst_ref=det.at[:, pl.ds(length, HALF)],
        send_sem=head_send, recv_sem=head_recv,
        device_id={"tm": left}, device_id_type=MESH,
    )

    @pl.when(jnp.logical_not(is_first))
    def _():
        head.start()


    for b in range(blocks):
        lanes = pl.ds(b * BLOCK, BLOCK)
        for k, piece in enumerate(parts_of(det[:, lanes])):
            split[k, :, lanes] = piece
    fetch.wait()
    lane = lax.broadcasted_iota(jnp.int32, (BLOCK, HALF), 1)
    depth = lax.broadcasted_iota(jnp.int32, (BLOCK, HALF), 0)
    for i in range(boxes):
        inside = (depth >= lane) & (depth < lane + widths[i])
        for k in range(3):
            box_band[pl.ds(k * BLOCK, BLOCK), pl.ds(i * HALF, HALF)] = inside.astype(
                jnp.float32
            ).astype(jnp.bfloat16)

    def lanes_of(i, t):
        return pl.ds((i * tiles + t) * HALF, HALF)

    def box_sums(t):
        window = jnp.concatenate(
            [split[k, :, pl.ds(t * HALF, BLOCK)] for k in range(3)], axis=1
        )
        sums = jnp.dot(window, box_band[...], preferred_element_type=jnp.float32)
        for i in range(boxes):
            boxed[:, lanes_of(i, t)] = sums[:, i * HALF:(i + 1) * HALF]

    for t in range(tiles - 1):
        box_sums(t)

    @pl.when(dm != dm_hub)
    def _():
        pl.semaphore_wait(dm_known, 1)

    pltpu.make_async_copy(power_in, power_in, power_recv).wait()
    totals = power_out[...] + jnp.sum(power_in[...], axis=0)
    inverse_scale = 1.0 / jnp.sqrt(totals * (1.0 / total_len) + EPS)
    for h in range(rows // HALF):
        row = jnp.broadcast_to(inverse_scale[h:h + 1, :], (HALF, HALF))
        scale[pl.ds(h * HALF, HALF), :] = row.T

    @pl.when(jnp.logical_not(is_last))
    def _():
        head.wait_recv()

    det[:, pl.ds(length, HALF)] = jnp.where(is_last, 0.0, det[:, pl.ds(length, HALF)])
    sums = [jnp.zeros((8, HALF), jnp.float32) for _ in range(tiles + 1)]
    for r in range(rows // 8):
        gain = scale[pl.ds(r * 8, 8), :]
        for t in range(tiles + 1):
            sums[t] = sums[t] + det[pl.ds(r * 8, 8), pl.ds(t * HALF, HALF)] * gain
    for t in range(tiles + 1):
        col_out[pl.ds(t, 1), :] = jnp.sum(sums[t], axis=0, keepdims=True)
    for k in range(dm_size - 1):
        later = jnp.where(dm <= k, 1, 0)
        pltpu.make_async_remote_copy(
            src_ref=col_out, dst_ref=col_in.at[dm - 1 + later],
            send_sem=col_send, recv_sem=col_recv,
            device_id={"dm": k + later}, device_id_type=MESH,
        ).start()

    for k, piece in enumerate(parts_of(det[:, pl.ds(length, HALF)])):
        split[k, :, pl.ds(length, HALF)] = piece
    box_sums(tiles - 1)

    inverse = []
    for i in range(boxes):
        width = jnp.full((8, HALF), widths[i], jnp.int32).astype(jnp.float32)
        inverse.append(1.0 / jnp.sqrt(width))

    def scale_rows(r, carry):
        span = pl.ds(pl.multiple_of(r * 8, 8), 8)
        gain = scale[span, :]
        for i in range(boxes):
            gain_i = gain * inverse[i]
            for t in range(tiles):
                boxed[span, lanes_of(i, t)] = boxed[span, lanes_of(i, t)] * gain_i
        return carry

    lax.fori_loop(0, rows // 8, scale_rows, 0)

    pltpu.make_async_copy(col_in, col_in, col_recv).wait()
    column_total = col_out[...] + jnp.sum(col_in[...], axis=0)
    common[...] = column_total * (1.0 / (rows * dm_size))
    window = jnp.concatenate([common[pl.ds(0, tiles), :], common[pl.ds(1, tiles), :]], axis=1)
    box_common[...] = banded(window, box_band[pl.ds(0, BLOCK), :])

    halves = rows // HALF
    offsets = [
        [
            jnp.broadcast_to(box_common[pl.ds(t, 1), pl.ds(i * HALF, HALF)], (8, HALF)) * inverse[i]
            for t in range(tiles)
        ]
        for i in range(boxes)
    ]

    def series_of(i, t, span):
        return boxed[span, lanes_of(i, t)] - offsets[i][t]

    for i in range(boxes):
        for h in range(halves):
            pieces = []
            for r in range(HALF // 8):
                span = pl.ds(h * HALF + r * 8, 8)
                values = [series_of(i, t, span) for t in range(tiles)]
                while len(values) > 1:
                    values = [jnp.maximum(a, b) for a, b in zip(values[::2], values[1::2])]
                pieces.append(values[0])
            turned = jnp.concatenate(pieces, axis=0).T
            peak_out[pl.ds(i * halves + h, 1), :] = jnp.max(turned, axis=0, keepdims=True)
    to_all(peak_out, peak_in, peak_send, peak_recv, places)

    for i in range(boxes):

        def some_rows(r, carry):
            top = pl.ds(pl.multiple_of(r * 16, 16), 8)
            bottom = pl.ds(pl.multiple_of(r * 16 + 8, 8), 8)
            both = pl.ds(pl.multiple_of(r * 16, 16), 16)
            for t in range(tiles):
                pair = jnp.concatenate([series_of(i, t, top), series_of(i, t, bottom)], axis=0)
                snr[i, both, pl.ds(t * HALF, HALF)] = pair.astype(jnp.bfloat16)
            return carry

        lax.fori_loop(0, rows // 16, some_rows, 0)

    pltpu.make_async_copy(peak_in, peak_in, peak_recv).wait()
    most = jnp.maximum(peak_out[...], jnp.max(peak_in[...], axis=0))
    for i in range(boxes):
        for h in range(halves):
            row = i * halves + h
            peaks[pl.ds(i, 1), pl.ds(h * HALF, HALF)] = most[row:row + 1, :]

    @pl.when(jnp.logical_not(is_last))
    def _():
        for copy in to_right:
            copy.wait_send()

    @pl.when(jnp.logical_not(is_first))
    def _():
        for copy in to_left:
            copy.wait_send()
        head.wait_send()

    pltpu.make_async_copy(power_in, power_in, power_send).wait()
    pltpu.make_async_copy(col_in, col_in, col_send).wait()
    pltpu.make_async_copy(peak_in, peak_in, peak_send).wait()


def hand_out(snr, peaks, snr_out, peaks_out, peaks_sem, sems):
    boxes, pieces = sems.shape
    rows = snr.shape[1] // pieces
    copies = [pltpu.make_async_copy(peaks, peaks_out, peaks_sem)]
    for i in range(boxes):
        for k in range(pieces):
            span = pl.ds(k * rows, rows)
            copies.append(pltpu.make_async_copy(snr.at[i, span], snr_out.at[i, span], sems.at[i, k]))
    for copy in copies:
        copy.start()
    for copy in copies:
        copy.wait()


def solution(mesh):
    tm_size, dm_size = mesh.shape["tm"], mesh.shape["dm"]

    def step(dispersed, widths):
        rows, length = dispersed.shape
        boxes = widths.shape[0]
        blocks, tiles, halves = length // BLOCK, length // HALF, rows // HALF
        f32, bf16 = jnp.float32, jnp.bfloat16
        dma = pltpu.SemaphoreType.DMA
        inputs = [pltpu.with_memory_space_constraint(a, pltpu.HBM) for a in (widths, dispersed)]
        snr, peaks = pl.pallas_call(
            functools.partial(kernel, tm_size, dm_size),
            out_shape=(
                pltpu.VMEM((boxes, rows, length), bf16),
                pltpu.VMEM((boxes, rows), f32),
            ),
            in_specs=[pl.BlockSpec(memory_space=pltpu.HBM)] * 2,
            out_specs=(pl.BlockSpec(memory_space=pltpu.VMEM),) * 2,
            scratch_shapes=[
                pltpu.SMEM((boxes,), jnp.int32),
                dma,
                pltpu.VMEM((blocks + 2, rows, BLOCK), f32),
                pltpu.VMEM((BLOCK, BLOCK), bf16),
                pltpu.VMEM((BLOCK, BLOCK), bf16),
                pltpu.VMEM((BLOCK, BLOCK), bf16),
                pltpu.VMEM((BLOCK, BLOCK), bf16),
                pltpu.VMEM((3 * BLOCK, boxes * HALF), bf16),
                pltpu.VMEM((blocks, rows, BLOCK), f32),
                pltpu.VMEM((2, rows, BLOCK), f32),
                pltpu.VMEM((rows, length + HALF), f32),
                pltpu.VMEM((3, rows, length + HALF), bf16),
                pltpu.VMEM((rows, boxes * tiles * HALF), f32),
                pltpu.VMEM((rows, HALF), f32),
                pltpu.VMEM((halves, HALF), f32),
                pltpu.VMEM((tm_size - 1, halves, HALF), f32),
                pltpu.VMEM((rows, HALF), f32),
                pltpu.VMEM((tiles + 1, HALF), f32),
                pltpu.VMEM((dm_size - 1, tiles + 1, HALF), f32),
                pltpu.VMEM((tiles + 1, HALF), f32),
                pltpu.VMEM((tiles, boxes * HALF), f32),
                pltpu.VMEM((boxes * halves, HALF), f32),
                pltpu.VMEM((tm_size - 1, boxes * halves, HALF), f32),
                dma((2, len(CHUNKS))),
                dma((blocks,)),
                dma((2, len(CHUNKS))),
                dma((2, len(CHUNKS))),
                dma, dma, dma, dma, dma, dma, dma, dma,
                pltpu.SemaphoreType.REGULAR,
                pltpu.SemaphoreType.REGULAR,
            ],
            compiler_params=pltpu.CompilerParams(
                collective_id=0, has_side_effects=True, vmem_limit_bytes=48 * 2**20
            ),
        )(*inputs)
        return pl.pallas_call(
            hand_out,
            out_shape=(
                jax.ShapeDtypeStruct(snr.shape, bf16),
                jax.ShapeDtypeStruct(peaks.shape, f32),
            ),
            in_specs=[pl.BlockSpec(memory_space=pl.ANY)] * 2,
            out_specs=(pl.BlockSpec(memory_space=pl.ANY),) * 2,
            scratch_shapes=[dma, dma((boxes, 1))],
            compiler_params=pltpu.CompilerParams(vmem_limit_bytes=2**22),
        )(snr, peaks)

    return jax.shard_map(
        step,
        mesh=mesh,
        in_specs=(P("dm", "tm"), P()),
        out_specs=(P(None, "dm", "tm"), P(None, "dm")),
        check_vma=False,
    )
```
